32 devices in a mesh: gx: 4 (over y, x), gy: 2 (over core), gz: 4 (over z).
Axes of the slice: x: 2, y: 2, z: 4, core: 2. Of those that a mesh axis runs over, the one named last changes fastest.
Arguments:
- energy: float32 [128, 256, 256], P(('gz', 'gy', 'gx')), may hold values from -5 to 5
- flow: float32 [4, 128, 256, 256], P(None, ('gz', 'gy', 'gx')), may hold values from -0.1 to 0.12, as said below
Outputs:
- energy_next: float32 [128, 256, 256], P('gz', 'gx', 'gy')
- plane_mean: float32 [128], P('gz')
- running_mean: float32 [128], P('gz')
The draws below stay inside these ranges and needn't reach their ends.
Inputs may be any that keep to these rules, and one draw needn't show every extreme that they name: flow[0], flow[1] and flow[2] lie within -0.1 to 0.1; flow[3] lies within 0.02 to 0.12.
All inputs are finite; a program needn't handle non-finite values.
Results may differ from the reference program's by a relative error of at most 0.00002.
Values sent between devices are 32-bit elements; how exact they have to be, the bound alone decides.
A program may use at most 128 MiB of HBM per device.

```python
import math
import jax
import jax.numpy as jnp

NX = 256
NY = 256
NZ = 128


def draw_energy(key, part):
    noise_key, phase_key, offset_key = jax.random.split(jax.random.fold_in(key, 11), 3)
    phases = jax.random.uniform(phase_key, (3,), jnp.float32, 0.0, 2.0 * math.pi)
    z_fraction = (jnp.arange(NZ, dtype=jnp.float32) / NZ)[:, None, None]
    x_fraction = (jnp.arange(NX, dtype=jnp.float32) / NX)[None, :, None]
    y_fraction = (jnp.arange(NY, dtype=jnp.float32) / NY)[None, None, :]
    offsets = jax.random.uniform(offset_key, (NZ, 1, 1), jnp.float32, -1.2, 1.2)
    smooth = offsets + 0.6 * jnp.sin(2.0 * math.pi * x_fraction + phases[0]) * jnp.cos(2.0 * math.pi * z_fraction + phases[1]) + 0.3 * jnp.cos(2.0 * math.pi * y_fraction + phases[2])
    noise = 0.8 * jnp.clip(jax.random.normal(noise_key, (NZ, NX, NY), jnp.float32), -3.0, 3.0)
    return (smooth + noise).astype(jnp.float32)


def draw_flow(key, part):
    speed_key, kappa_key = jax.random.split(jax.random.fold_in(key, 23))
    speeds = jax.random.uniform(speed_key, (3, NZ, NX, NY), jnp.float32, -0.1, 0.1)
    conductivity = jnp.exp(jax.random.uniform(kappa_key, (1, NZ, NX, NY), jnp.float32, math.log(0.02), math.log(0.12)))
    return jnp.concatenate([speeds, conductivity], 0).astype(jnp.float32)


def setup_inputs(seed: int = 0) -> dict:
    seeds = jax.random.split(jax.random.key(seed), 3)
    return {
        "energy": draw_energy(jax.random.fold_in(seeds[2], 71), 0),
        "flow": draw_flow(jax.random.fold_in(seeds[2], 71), 0),
    }


directions = ((1, 0, 0), (0, 1, 0), (0, 0, 1))


def extend(field):
    padded = jnp.pad(field, ((0, 0), (1, 1), (1, 1)))
    return jnp.concatenate([padded[-1:], padded, padded[:1]], 0)


def window(array, offset):
    return array[1 + offset[0]: array.shape[0] - 1 + offset[0],
                 1 + offset[1]: array.shape[1] - 1 + offset[1],
                 1 + offset[2]: array.shape[2] - 1 + offset[2]]


def advance(energy_pad, kappa_pad, velocity):
    centre = window(energy_pad, (0, 0, 0))
    kappa_centre = window(kappa_pad, (0, 0, 0))
    change = jnp.zeros_like(centre)
    for axis_number, forward in enumerate(directions):
        backward = tuple(-item for item in forward)
        upper = window(energy_pad, forward)
        lower = window(energy_pad, backward)
        kappa_upper = window(kappa_pad, forward)
        kappa_lower = window(kappa_pad, backward)
        change = change + 0.5 * (kappa_centre + kappa_upper) * (upper - centre) - 0.5 * (kappa_centre + kappa_lower) * (centre - lower)
        speed = velocity[axis_number]
        change = change - jnp.maximum(speed, 0.0) * (centre - lower) - jnp.minimum(speed, 0.0) * (upper - centre)
    return centre + change


def reference(energy, flow):
    velocity = flow[:3]
    kappa_pad = extend(flow[3])
    energy_half = advance(extend(energy), kappa_pad, velocity)
    energy_next = advance(extend(energy_half), kappa_pad, velocity)
    plane_mean = jnp.sum(energy_next, axis=(1, 2)) / (NX * NY)
    ranks = jnp.arange(1, NZ + 1).astype(jnp.float32)
    running_mean = jnp.cumsum(plane_mean) / ranks
    return energy_next, plane_mean, running_mean
```

```python
import functools

import jax
import jax.numpy as jnp
from jax import lax
from jax.experimental import pallas as pl
from jax.experimental.pallas import tpu as pltpu
from jax.sharding import PartitionSpec as P

MESH = pl.DeviceIdType.MESH
PAD = 8
ROWS = 16
STRIP = 32


def shifted(block, rows):
    size = block.shape[0]
    return (
        block[PAD : PAD + rows],
        pltpu.roll(block, size - 1, 0)[PAD : PAD + rows],
        pltpu.roll(block, 1, 0)[PAD : PAD + rows],
    )


def sideways(block, lane):
    width = block.shape[1]
    right = jnp.where(lane == width - 1, 0.0, pltpu.roll(block, width - 1, 1))
    left = jnp.where(lane == 0, 0.0, pltpu.roll(block, 1, 1))
    return right, left


def above(k, k_up, speed, e, e_up):
    return (0.5 * (k + k_up) - jnp.minimum(speed, 0.0)) * (e_up - e)


def below(k, k_down, speed, e, e_down):
    return (0.5 * (k + k_down) + jnp.maximum(speed, 0.0)) * (e_down - e)


def kernel(
    sizes, e_hbm, f_hbm, out, mean_ref, run_ref,
    e_v, k_v, u_v, h_v, n_v, group_v, block_v,
    load_sem, s1, r1, s2, r2, s3, r3, own_sem, s4, r4, s5, r5,
):
    gx_n, gy_n, gz_n, planes, nx, ny = sizes
    height, width = nx // gx_n, ny // gy_n
    gx, gy, gz = lax.axis_index("gx"), lax.axis_index("gy"), lax.axis_index("gz")
    peers = gx_n * gy_n
    place = gy * gx_n + gx
    slab = gz * peers + place

    def device(number):
        return {
            "gx": lax.rem(number, gx_n),
            "gy": lax.rem(lax.div(number, gx_n), gy_n),
            "gz": lax.div(number, peers),
        }

    total = peers * gz_n
    up = device(lax.rem(slab + 1, total))
    down = device(lax.rem(slab + total - 1, total))

    def peer(step):
        return {
            "gx": lax.rem(place + step, gx_n) if gy_n == 1 else lax.rem(lax.rem(place + step, peers), gx_n),
            "gy": lax.div(lax.rem(place + step, peers), gx_n),
            "gz": gz,
        }

    def layer(step):
        return {"gx": gx, "gy": gy, "gz": lax.rem(gz + step, gz_n)}

    loads = [
        pltpu.make_async_copy(e_hbm, e_v.at[pl.ds(1, planes), pl.ds(PAD, nx)], load_sem.at[0]),
        pltpu.make_async_copy(f_hbm.at[3], k_v.at[pl.ds(1, planes), pl.ds(PAD, nx)], load_sem.at[1]),
        pltpu.make_async_copy(f_hbm.at[pl.ds(0, 3)], u_v, load_sem.at[2]),
    ]

    barrier = pltpu.get_barrier_semaphore()
    greet = [up, down] + [peer(i) for i in range(1, peers)] + [layer(i) for i in range(1, gz_n)]
    for target in greet:
        pl.semaphore_signal(barrier, inc=1, device_id=target, device_id_type=MESH)
    for load in loads:
        load.start()
    edge = jnp.zeros((planes, PAD, ny), jnp.float32)
    for ref in (e_v, k_v, h_v):
        ref[1 : planes + 1, 0:PAD, :] = edge
        ref[1 : planes + 1, PAD + nx : PAD + nx + PAD, :] = edge
    pl.semaphore_wait(barrier, len(greet))

    def lanes(c):
        return pl.ds(c * width, width)

    def send(src, dst, send_sem, recv_sem, target):
        return pltpu.make_async_remote_copy(
            src_ref=src, dst_ref=dst, send_sem=send_sem, recv_sem=recv_sem,
            device_id=target, device_id_type=MESH,
        )

    first = []
    rows_all = pl.ds(PAD, nx)
    for c in range(gy_n):
        copies = [
            send(e_hbm.at[planes - 1, :, lanes(c)], e_v.at[0, rows_all, lanes(c)], s1.at[c, 0], r1.at[c, 0], up),
            send(e_hbm.at[0, :, lanes(c)], e_v.at[planes + 1, rows_all, lanes(c)], s1.at[c, 1], r1.at[c, 1], down),
            send(f_hbm.at[3, planes - 1, :, lanes(c)], k_v.at[0, rows_all, lanes(c)], s1.at[c, 2], r1.at[c, 2], up),
            send(f_hbm.at[3, 0, :, lanes(c)], k_v.at[planes + 1, rows_all, lanes(c)], s1.at[c, 3], r1.at[c, 3], down),
        ]
        for copy in copies:
            copy.start()
        first.append(copies)

    for load in loads:
        load.wait()

    lane = lax.broadcasted_iota(jnp.int32, (ROWS, ny), 1)

    def local(src, p, r):
        start = pl.multiple_of(r * ROWS, ROWS)
        here = pl.ds(start, ROWS)
        inner = pl.ds(pl.multiple_of(start + PAD, PAD), ROWS)
        tall = pl.ds(start, ROWS + 2 * PAD)
        e, e_next, e_prev = shifted(src[p + 1, tall, :], ROWS)
        k, k_next, k_prev = shifted(k_v[p + 1, tall, :], ROWS)
        speed = u_v[1, p, here, :]
        value = e + above(k, k_next, speed, e, e_next) + below(k, k_prev, speed, e, e_prev)
        e_next, e_prev = sideways(e, lane)
        k_next, k_prev = sideways(k, lane)
        speed = u_v[2, p, here, :]
        value = value + above(k, k_next, speed, e, e_next) + below(k, k_prev, speed, e, e_prev)
        speed = u_v[0, p, here, :]
        if p < planes - 1:
            value = value + above(k, k_v[p + 2, inner, :], speed, e, src[p + 2, inner, :])
        if p > 0:
            value = value + below(k, k_v[p, inner, :], speed, e, src[p, inner, :])
        return here, inner, value

    def edge_terms(src, c, r):
        start = pl.multiple_of(r * STRIP, STRIP)
        here = pl.ds(start, STRIP)
        inner = pl.ds(pl.multiple_of(start + PAD, PAD), STRIP)
        at = lanes(c)
        top = above(
            k_v[planes, inner, at], k_v[planes + 1, inner, at], u_v[0, planes - 1, here, at],
            src[planes, inner, at], src[planes + 1, inner, at],
        )
        bottom = below(
            k_v[1, inner, at], k_v[0, inner, at], u_v[0, 0, here, at], src[1, inner, at], src[0, inner, at]
        )
        return here, inner, top, bottom

    def folded(value):
        rows = value.shape[0]
        part = value[0:8]
        for i in range(8, rows, 8):
            part = part + value[i : i + 8]
        return part

    for p in range(planes):

        @pl.loop(0, nx // ROWS)
        def _(r, p=p):
            here, inner, value = local(e_v, p, r)
            h_v[p + 1, inner, :] = value

    second = []
    for c in range(gy_n):
        for copy in first[c]:
            copy.wait_recv()

        @pl.loop(0, nx // STRIP)
        def _(r, c=c):
            here, inner, top, bottom = edge_terms(e_v, c, r)
            h_v[planes, inner, lanes(c)] = h_v[planes, inner, lanes(c)] + top
            h_v[1, inner, lanes(c)] = h_v[1, inner, lanes(c)] + bottom

        copies = [
            send(h_v.at[planes, rows_all, lanes(c)], h_v.at[0, rows_all, lanes(c)], s2.at[c, 0], r2.at[c, 0], up),
            send(h_v.at[1, rows_all, lanes(c)], h_v.at[planes + 1, rows_all, lanes(c)], s2.at[c, 1], r2.at[c, 1], down),
        ]
        for copy in copies:
            copy.start()
        second.append(copies)

    sums = []
    for p in range(planes):

        def body(r, carry, p=p):
            here, inner, value = local(h_v, p, r)
            n_v[p, here, :] = value
            return carry + folded(value)

        sums.append(lax.fori_loop(0, nx // ROWS, body, jnp.zeros((8, ny), jnp.float32)))

    def hand_out(c, p0, count, part):
        for d in range(gx_n):
            to = lax.rem(gx + d, gx_n)
            src = n_v.at[pl.ds(p0, count), pl.ds(pl.multiple_of(to * height, 8), height), lanes(c)]
            dst = out.at[pl.ds(place * planes + p0, count)]
            if d == 0:

                @pl.when(gy == c)
                def _():
                    pltpu.make_async_copy(src, dst, own_sem.at[part]).start()

                @pl.when(gy != c)
                def _():
                    send(src, dst, s3.at[c * gx_n + d, part], r3.at[place, part],
                         {"gx": gx, "gy": jnp.int32(c), "gz": gz}).start()
            else:
                send(src, dst, s3.at[c * gx_n + d, part], r3.at[place, part],
                     {"gx": to, "gy": jnp.int32(c), "gz": gz}).start()

    parts = []
    if planes > 2:
        parts.append((1, planes - 2))
        for c in range(gy_n):
            hand_out(c, 1, planes - 2, 0)
    outer = sorted({0, planes - 1})
    first_outer = len(parts)
    parts += [(p, 1) for p in outer]

    extra = [jnp.zeros((8, width), jnp.float32), jnp.zeros((8, width), jnp.float32)]
    for c in range(gy_n):
        for copy in second[c]:
            copy.wait_recv()

        def body(r, carry, c=c):
            here, inner, top, bottom = edge_terms(h_v, c, r)
            n_v[planes - 1, here, lanes(c)] = n_v[planes - 1, here, lanes(c)] + top
            n_v[0, here, lanes(c)] = n_v[0, here, lanes(c)] + bottom
            return carry[0] + folded(top), carry[1] + folded(bottom)

        extra = lax.fori_loop(0, nx // STRIP, body, tuple(extra))
        for part, p in enumerate(outer):
            hand_out(c, p, 1, first_outer + part)

    spot = lax.broadcasted_iota(jnp.int32, (8, 128), 1)
    mine = jnp.zeros((8, 128), jnp.float32)
    for p in range(planes):
        amount = jnp.sum(sums[p], keepdims=True)
        if p == planes - 1:
            amount = amount + jnp.sum(extra[0], keepdims=True)
        if p == 0:
            amount = amount + jnp.sum(extra[1], keepdims=True)
        mine = jnp.where(spot == place * planes + p, amount * (1.0 / (nx * ny)), mine)
    group_v[0] = mine
    share = []
    for i in range(1, peers):
        copy = send(group_v.at[0], group_v.at[i], s4.at[i], r4.at[i], peer(i))
        copy.start()
        share.append(copy)
    for copy in share:
        copy.wait_recv()
    means = mine
    for i in range(1, peers):
        means = means + group_v[i]
    block_v[0] = means
    climb = []
    for i in range(1, gz_n):
        copy = send(block_v.at[0], block_v.at[i], s5.at[i], r5.at[i], layer(i))
        copy.start()
        climb.append(copy)
    running = means
    step = 1
    while step < peers * planes:
        running = running + jnp.where(spot >= step, pltpu.roll(running, step, 1), 0.0)
        step *= 2
    mean_ref[...] = means
    for copy in climb:
        copy.wait_recv()
    lower = jnp.zeros((8, 128), jnp.float32)
    for i in range(1, gz_n):
        lower = lower + jnp.where(gz >= i, block_v[i], 0.0)
    offset = jnp.sum(lower[0:1], axis=1, keepdims=True)
    rank = (gz * peers * planes + spot + 1).astype(jnp.float32)
    run_ref[...] = (running + offset) / rank

    for part, (p0, count) in enumerate(parts):
        for d in range(peers):
            source = lax.rem(place + d, peers)
            dst = out.at[pl.ds(source * planes + p0, count)]
            src = n_v.at[pl.ds(p0, count), pl.ds(0, height), pl.ds(0, width)]
            if d == 0:
                pltpu.make_async_copy(src, dst, own_sem.at[part]).wait()
            else:
                send(src, dst, s3.at[0, part], r3.at[source, part], peer(d)).wait_recv()
        for c in range(gy_n):
            for d in range(gx_n):
                copy = send(
                    n_v.at[pl.ds(p0, count), pl.ds(0, height), pl.ds(0, width)],
                    out.at[pl.ds(p0, count)], s3.at[c * gx_n + d, part], r3.at[0, part], up,
                )
                if d == 0:

                    @pl.when(gy != c)
                    def _():
                        copy.wait_send()
                else:
                    copy.wait_send()
    for copies in first + second + [share, climb]:
        for copy in copies:
            copy.wait_send()


def per_device(energy, flow):
    gx_n, gy_n, gz_n = (lax.axis_size(a) for a in ("gx", "gy", "gz"))
    planes, nx, ny = energy.shape
    peers = gx_n * gy_n
    parts = (1 if planes > 2 else 0) + (2 if planes > 1 else 1)
    dma = pltpu.SemaphoreType.DMA
    f32 = jnp.float32
    anywhere = pl.BlockSpec(memory_space=pl.ANY)
    vmem = pl.BlockSpec(memory_space=pltpu.VMEM)
    tall = pltpu.VMEM((planes + 2, nx + 2 * PAD, ny), f32)
    energy_next, means, running = pl.pallas_call(
        functools.partial(kernel, (gx_n, gy_n, gz_n, planes, nx, ny)),
        out_shape=(
            jax.ShapeDtypeStruct((planes * peers, nx // gx_n, ny // gy_n), f32),
            jax.ShapeDtypeStruct((8, 128), f32),
            jax.ShapeDtypeStruct((8, 128), f32),
        ),
        in_specs=[anywhere, anywhere],
        out_specs=(anywhere, vmem, vmem),
        scratch_shapes=[
            tall, tall, pltpu.VMEM((3, planes, nx, ny), f32), tall,
            pltpu.VMEM((planes, nx, ny), f32),
            pltpu.VMEM((peers, 8, 128), f32), pltpu.VMEM((gz_n, 8, 128), f32),
            dma((3,)), dma((gy_n, 4)), dma((gy_n, 4)), dma((gy_n, 2)), dma((gy_n, 2)),
            dma((peers, parts)), dma((peers, parts)), dma((parts,)),
            dma((peers,)), dma((peers,)), dma((gz_n,)), dma((gz_n,)),
        ],
        compiler_params=pltpu.CompilerParams(collective_id=0, has_side_effects=True),
    )(energy, flow)
    count = planes * peers
    return energy_next, means[0, :count], running[0, :count]


def solution(mesh):
    placed = (P(("gz", "gy", "gx"), None, None), P(None, ("gz", "gy", "gx"), None, None))
    return jax.shard_map(
        per_device,
        mesh=mesh,
        in_specs=placed,
        out_specs=(P("gz", "gx", "gy"), P("gz"), P("gz")),
        check_vma=False,
    )
```

```python
import functools

import jax
import jax.numpy as jnp
from jax import lax
from jax.experimental import pallas as pl
from jax.experimental.pallas import tpu as pltpu
from jax.sharding import PartitionSpec as P

MESH = pl.DeviceIdType.MESH
PAD = 8
ROWS = 16
STRIP = 32


def shifted(block, rows):
    size = block.shape[0]
    return (
        block[PAD : PAD + rows],
        pltpu.roll(block, size - 1, 0)[PAD : PAD + rows],
        pltpu.roll(block, 1, 0)[PAD : PAD + rows],
    )


def sideways(block, lane):
    width = block.shape[1]
    right = jnp.where(lane == width - 1, 0.0, pltpu.roll(block, width - 1, 1))
    left = jnp.where(lane == 0, 0.0, pltpu.roll(block, 1, 1))
    return right, left


def above(k, k_up, speed, e, e_up):
    return (0.5 * (k + k_up) - jnp.minimum(speed, 0.0)) * (e_up - e)


def below(k, k_down, speed, e, e_down):
    return (0.5 * (k + k_down) + jnp.maximum(speed, 0.0)) * (e_down - e)


def kernel(
    sizes, e_hbm, f_hbm, out, mean_ref, run_ref,
    e_v, k_v, u_v, h_v, n_v, group_v, block_v,
    load_sem, s1, r1, s2, r2, s3, r3, own_sem, s4, r4, s5, r5,
):
    gx_n, gy_n, gz_n, planes, nx, ny = sizes
    height, width = nx // gx_n, ny // gy_n
    gx, gy, gz = lax.axis_index("gx"), lax.axis_index("gy"), lax.axis_index("gz")
    peers = gx_n * gy_n
    place = gy * gx_n + gx
    slab = gz * peers + place

    def device(number):
        return {
            "gx": lax.rem(number, gx_n),
            "gy": lax.rem(lax.div(number, gx_n), gy_n),
            "gz": lax.div(number, peers),
        }

    total = peers * gz_n
    up = device(lax.rem(slab + 1, total))
    down = device(lax.rem(slab + total - 1, total))

    def peer(step):
        return {
            "gx": lax.rem(place + step, gx_n) if gy_n == 1 else lax.rem(lax.rem(place + step, peers), gx_n),
            "gy": lax.div(lax.rem(place + step, peers), gx_n),
            "gz": gz,
        }

    def layer(step):
        return {"gx": gx, "gy": gy, "gz": lax.rem(gz + step, gz_n)}

    loads = [
        pltpu.make_async_copy(e_hbm, e_v.at[pl.ds(1, planes), pl.ds(PAD, nx)], load_sem.at[0]),
        pltpu.make_async_copy(f_hbm.at[3], k_v.at[pl.ds(1, planes), pl.ds(PAD, nx)], load_sem.at[1]),
        pltpu.make_async_copy(f_hbm.at[pl.ds(0, 3)], u_v, load_sem.at[2]),
    ]

    barrier = pltpu.get_barrier_semaphore()
    greet = [up, down] + [peer(i) for i in range(1, peers)] + [layer(i) for i in range(1, gz_n)]
    for target in greet:
        pl.semaphore_signal(barrier, inc=1, device_id=target, device_id_type=MESH)
    for load in loads:
        load.start()
    edge = jnp.zeros((planes, PAD, ny), jnp.float32)
    for ref in (e_v, k_v, h_v):
        ref[1 : planes + 1, 0:PAD, :] = edge
        ref[1 : planes + 1, PAD + nx : PAD + nx + PAD, :] = edge
    pl.semaphore_wait(barrier, len(greet))

    def lanes(c):
        return pl.ds(c * width, width)

    def send(src, dst, send_sem, recv_sem, target):
        return pltpu.make_async_remote_copy(
            src_ref=src, dst_ref=dst, send_sem=send_sem, recv_sem=recv_sem,
            device_id=target, device_id_type=MESH,
        )

    first = []
    rows_all = pl.ds(PAD, nx)
    for c in range(gy_n):
        copies = [
            send(e_hbm.at[planes - 1, :, lanes(c)], e_v.at[0, rows_all, lanes(c)], s1.at[c, 0], r1.at[c, 0], up),
            send(e_hbm.at[0, :, lanes(c)], e_v.at[planes + 1, rows_all, lanes(c)], s1.at[c, 1], r1.at[c, 1], down),
            send(f_hbm.at[3, planes - 1, :, lanes(c)], k_v.at[0, rows_all, lanes(c)], s1.at[c, 2], r1.at[c, 2], up),
            send(f_hbm.at[3, 0, :, lanes(c)], k_v.at[planes + 1, rows_all, lanes(c)], s1.at[c, 3], r1.at[c, 3], down),
        ]
        for copy in copies:
            copy.start()
        first.append(copies)

    for load in loads:
        load.wait()

    lane = lax.broadcasted_iota(jnp.int32, (ROWS, ny), 1)

    def local(src, p, r):
        start = pl.multiple_of(r * ROWS, ROWS)
        here = pl.ds(start, ROWS)
        inner = pl.ds(pl.multiple_of(start + PAD, PAD), ROWS)
        tall = pl.ds(start, ROWS + 2 * PAD)
        e, e_next, e_prev = shifted(src[p + 1, tall, :], ROWS)
        k, k_next, k_prev = shifted(k_v[p + 1, tall, :], ROWS)
        speed = u_v[1, p, here, :]
        value = e + above(k, k_next, speed, e, e_next) + below(k, k_prev, speed, e, e_prev)
        e_next, e_prev = sideways(e, lane)
        k_next, k_prev = sideways(k, lane)
        speed = u_v[2, p, here, :]
        value = value + above(k, k_next, speed, e, e_next) + below(k, k_prev, speed, e, e_prev)
        speed = u_v[0, p, here, :]
        if p < planes - 1:
            value = value + above(k, k_v[p + 2, inner, :], speed, e, src[p + 2, inner, :])
        if p > 0:
            value = value + below(k, k_v[p, inner, :], speed, e, src[p, inner, :])
        return here, inner, value

    def edge_terms(src, c, r):
        start = pl.multiple_of(r * STRIP, STRIP)
        here = pl.ds(start, STRIP)
        inner = pl.ds(pl.multiple_of(start + PAD, PAD), STRIP)
        at = lanes(c)
        top = above(
            k_v[planes, inner, at], k_v[planes + 1, inner, at], u_v[0, planes - 1, here, at],
            src[planes, inner, at], src[planes + 1, inner, at],
        )
        bottom = below(
            k_v[1, inner, at], k_v[0, inner, at], u_v[0, 0, here, at], src[1, inner, at], src[0, inner, at]
        )
        return here, inner, top, bottom

    def folded(value):
        rows = value.shape[0]
        part = value[0:8]
        for i in range(8, rows, 8):
            part = part + value[i : i + 8]
        return part

    for p in range(planes):

        @pl.loop(0, nx // ROWS)
        def _(r, p=p):
            here, inner, value = local(e_v, p, r)
            h_v[p + 1, inner, :] = value

    second = []
    for c in range(gy_n):
        for copy in first[c]:
            copy.wait_recv()

        @pl.loop(0, nx // STRIP)
        def _(r, c=c):
            here, inner, top, bottom = edge_terms(e_v, c, r)
            h_v[planes, inner, lanes(c)] = h_v[planes, inner, lanes(c)] + top
            h_v[1, inner, lanes(c)] = h_v[1, inner, lanes(c)] + bottom

        copies = [
            send(h_v.at[planes, rows_all, lanes(c)], h_v.at[0, rows_all, lanes(c)], s2.at[c, 0], r2.at[c, 0], up),
            send(h_v.at[1, rows_all, lanes(c)], h_v.at[planes + 1, rows_all, lanes(c)], s2.at[c, 1], r2.at[c, 1], down),
        ]
        for copy in copies:
            copy.start()
        second.append(copies)

    sums = []
    for p in range(planes):

        def body(r, carry, p=p):
            here, inner, value = local(h_v, p, r)
            n_v[p, here, :] = value
            return carry + folded(value)

        sums.append(lax.fori_loop(0, nx // ROWS, body, jnp.zeros((8, ny), jnp.float32)))

    def hand_out(c, p0, count, part):
        for d in range(gx_n):
            to = lax.rem(gx + d, gx_n)
            src = n_v.at[pl.ds(p0, count), pl.ds(pl.multiple_of(to * height, 8), height), lanes(c)]
            dst = out.at[pl.ds(place * planes + p0, count)]
            if d == 0:

                @pl.when(gy == c)
                def _():
                    pltpu.make_async_copy(src, dst, own_sem.at[part]).start()

                @pl.when(gy != c)
                def _():
                    send(src, dst, s3.at[c * gx_n + d, part], r3.at[place, part],
                         {"gx": gx, "gy": jnp.int32(c), "gz": gz}).start()
            else:
                send(src, dst, s3.at[c * gx_n + d, part], r3.at[place, part],
                     {"gx": to, "gy": jnp.int32(c), "gz": gz}).start()

    parts = []
    if planes > 2:
        parts.append((1, planes - 2))
        for c in range(gy_n):
            hand_out(c, 1, planes - 2, 0)
    outer = sorted({0, planes - 1})
    first_outer = len(parts)
    parts += [(p, 1) for p in outer]

    extra = [jnp.zeros((8, width), jnp.float32), jnp.zeros((8, width), jnp.float32)]
    for c in range(gy_n):
        for copy in second[c]:
            copy.wait_recv()

        def body(r, carry, c=c):
            here, inner, top, bottom = edge_terms(h_v, c, r)
            n_v[planes - 1, here, lanes(c)] = n_v[planes - 1, here, lanes(c)] + top
            n_v[0, here, lanes(c)] = n_v[0, here, lanes(c)] + bottom
            return carry[0] + folded(top), carry[1] + folded(bottom)

        extra = lax.fori_loop(0, nx // STRIP, body, tuple(extra))
        for part, p in enumerate(outer):
            hand_out(c, p, 1, first_outer + part)

    spot = lax.broadcasted_iota(jnp.int32, (8, 128), 1)
    mine = jnp.zeros((8, 128), jnp.float32)
    for p in range(planes):
        amount = jnp.sum(sums[p], keepdims=True)
        if p == planes - 1:
            amount = amount + jnp.sum(extra[0], keepdims=True)
        if p == 0:
            amount = amount + jnp.sum(extra[1], keepdims=True)
        mine = jnp.where(spot == place * planes + p, amount * (1.0 / (nx * ny)), mine)
    group_v[0] = mine
    share = []
    for i in range(1, peers):
        copy = send(group_v.at[0], group_v.at[i], s4.at[i], r4.at[i], peer(i))
        copy.start()
        share.append(copy)
    for copy in share:
        copy.wait_recv()
    means = mine
    for i in range(1, peers):
        means = means + group_v[i]
    block_v[0] = means
    climb = []
    for i in range(1, gz_n):
        copy = send(block_v.at[0], block_v.at[i], s5.at[i], r5.at[i], layer(i))
        copy.start()
        climb.append(copy)
    running = means
    step = 1
    while step < peers * planes:
        running = running + jnp.where(spot >= step, pltpu.roll(running, step, 1), 0.0)
        step *= 2
    mean_ref[...] = means
    for copy in climb:
        copy.wait_recv()
    lower = jnp.zeros((8, 128), jnp.float32)
    for i in range(1, gz_n):
        lower = lower + jnp.where(gz >= i, block_v[i], 0.0)
    offset = jnp.sum(lower[0:1], axis=1, keepdims=True)
    rank = (gz * peers * planes + spot + 1).astype(jnp.float32)
    run_ref[...] = (running + offset) / rank

    for part, (p0, count) in enumerate(parts):
        for d in range(peers):
            source = lax.rem(place + d, peers)
            dst = out.at[pl.ds(source * planes + p0, count)]
            src = n_v.at[pl.ds(p0, count), pl.ds(0, height), pl.ds(0, width)]
            if d == 0:
                pltpu.make_async_copy(src, dst, own_sem.at[part]).wait()
            else:
                send(src, dst, s3.at[0, part], r3.at[source, part], peer(d)).wait_recv()
        for c in range(gy_n):
            for d in range(gx_n):
                copy = send(
                    n_v.at[pl.ds(p0, count), pl.ds(0, height), pl.ds(0, width)],
                    out.at[pl.ds(p0, count)], s3.at[c * gx_n + d, part], r3.at[0, part], up,
                )
                if d == 0:

                    @pl.when(gy != c)
                    def _():
                        copy.wait_send()
                else:
                    copy.wait_send()
    for copies in first + second + [share, climb]:
        for copy in copies:
            copy.wait_send()


def split_kernel(
    sizes, e_hbm, f_hbm, out, corr, mean_ref, run_ref,
    e_v, k_v, u_v, h_v, n_v, g_v, rx_v, d_v, c_v, near_v, far_v, group_v, block_v,
    load_sem, s1, r1, s2, r2, s3, r3, sc, rc, s4, r4, s5, r5,
):
    gx_n, gy_n, gz_n, planes, nx, ny = sizes
    height, width = nx // gx_n, ny // gy_n
    halves = gx_n // 2
    gx, gy, gz = lax.axis_index("gx"), lax.axis_index("gy"), lax.axis_index("gz")
    peers = gx_n * gy_n
    count = peers * planes
    place = gy * gx_n + gx
    slab = gz * peers + place
    parity = lax.rem(gx, 2)
    total = peers * gz_n
    above_slab, below_slab = lax.rem(slab + 1, total), lax.rem(slab + total - 1, total)
    last = planes - 1
    own_plane = (0, last)

    def device(number):
        return {
            "gx": lax.rem(number, gx_n),
            "gy": lax.rem(lax.div(number, gx_n), gy_n),
            "gz": lax.div(number, peers),
        }

    neighbour = (device(below_slab), device(above_slab))

    def peer(step):
        return device(gz * peers + lax.rem(place + step, peers))

    def layer(step):
        return {"gx": gx, "gy": gy, "gz": lax.rem(gz + step, gz_n)}

    loads = [
        pltpu.make_async_copy(e_hbm, e_v.at[:, pl.ds(PAD, nx)], load_sem.at[0]),
        pltpu.make_async_copy(f_hbm.at[3], k_v.at[:, pl.ds(PAD, nx)], load_sem.at[1]),
        pltpu.make_async_copy(f_hbm.at[pl.ds(0, 3)], u_v, load_sem.at[2]),
    ]
    for load in loads:
        load.start()

    barrier = pltpu.get_barrier_semaphore()
    greet = list(neighbour) + [peer(i) for i in range(1, peers)] + [layer(i) for i in range(1, gz_n)]
    greet.append(device(lax.rem(gz + gz_n - 1, gz_n) * peers + peers - 1))
    greet.append(device(lax.rem(gz + 1, gz_n) * peers))
    for target in greet:
        pl.semaphore_signal(barrier, inc=1, device_id=target, device_id_type=MESH)
    edge = jnp.zeros((planes, PAD, ny), jnp.float32)
    for ref in (e_v, k_v, h_v):
        ref[:, 0:PAD, :] = edge
        ref[:, PAD + nx : PAD + nx + PAD, :] = edge
    outermost = (place == 0).astype(jnp.int32) + (place == peers - 1).astype(jnp.int32)
    pl.semaphore_wait(barrier, len(greet) - 2 + outermost * peers)

    def lanes(c):
        return pl.ds(c * width, width)

    def send(src, dst, send_sem, recv_sem, target):
        return pltpu.make_async_remote_copy(
            src_ref=src, dst_ref=dst, send_sem=send_sem, recv_sem=recv_sem,
            device_id=target, device_id_type=MESH,
        )

    def row(block, extra=0):
        return pl.multiple_of(block * height + extra, 8)

    mine = [2 * j + parity for j in range(halves)]
    theirs = [2 * j + 1 - parity for j in range(halves)]

    first = {}

    def start_first(j, fields):
        for f in (1, 0):
            p, rows = own_plane[f], pl.ds(row(theirs[j]), height)
            inner = pl.ds(row(theirs[j], PAD), height)
            sources = (e_hbm.at[p, rows], f_hbm.at[3, p, rows], g_v.at[f, rows], h_v.at[p, inner])
            for i in fields:
                copy = send(sources[i], rx_v.at[1 - f, i, j], s1.at[f, i, j], r1.at[1 - f, i, j], neighbour[f])
                copy.start()
                first[f, i, j] = copy

    start_first(0, (0, 1))
    for load in loads:
        load.wait()

    lane = lax.broadcasted_iota(jnp.int32, (ROWS, ny), 1)
    tiles = height // ROWS

    def local(src, p, start):
        here = pl.ds(start, ROWS)
        inner = pl.ds(pl.multiple_of(start + PAD, 8), ROWS)
        tall = pl.ds(start, ROWS + 2 * PAD)
        e, e_next, e_prev = shifted(src[p, tall, :], ROWS)
        k, k_next, k_prev = shifted(k_v[p, tall, :], ROWS)
        speed = u_v[1, p, here, :]
        value = e + above(k, k_next, speed, e, e_next) + below(k, k_prev, speed, e, e_prev)
        e_next, e_prev = sideways(e, lane)
        k_next, k_prev = sideways(k, lane)
        speed = u_v[2, p, here, :]
        value = value + above(k, k_next, speed, e, e_next) + below(k, k_prev, speed, e, e_prev)
        speed = u_v[0, p, here, :]
        if p < last:
            value = value + above(k, k_v[p + 1, inner, :], speed, e, src[p + 1, inner, :])
        if p > 0:
            value = value + below(k, k_v[p - 1, inner, :], speed, e, src[p - 1, inner, :])
        return here, inner, value, 0.5 * k, speed

    def folded(value):
        part = value[0:8]
        for i in range(8, value.shape[0], 8):
            part = part + value[i : i + 8]
        return part

    def first_step(block, which):
        @pl.loop(0, tiles)
        def _(t):
            start = pl.multiple_of(block * height + t * ROWS, 8)
            for p in which:
                here, inner, value, half, speed = local(e_v, p, start)
                h_v[p, inner, :] = value
                if p == 0:
                    g_v[0, here, :] = half + jnp.maximum(speed, 0.0)
                if p == last:
                    g_v[1, here, :] = half - jnp.minimum(speed, 0.0)

    for j in range(halves):
        if j > 0:
            start_first(j, (0, 1))
        first_step(theirs[j], own_plane)
        start_first(j, (2, 3))
    for j in range(halves):
        first_step(mine[j], own_plane)
    inside = tuple(range(1, last))
    if inside:
        for block in range(gx_n):
            first_step(block, inside)

    second, fixes = [], []
    side_slab = (below_slab, above_slab)
    zero = jnp.zeros((8, ny), jnp.float32)
    spill = (zero, zero)
    for j in range(halves):
        for f in (0, 1):
            for i in range(4):
                send(rx_v.at[f, i, j], rx_v.at[f, i, j], s1.at[f, i, j], r1.at[f, i, j], neighbour[f]).wait_recv()

        def body(t, carry, j=j):
            sums = []
            at = pl.ds(pl.multiple_of(t * ROWS, 8), ROWS)
            start = pl.multiple_of(mine[j] * height + t * ROWS, 8)
            here, inner = pl.ds(start, ROWS), pl.ds(pl.multiple_of(start + PAD, 8), ROWS)
            for f in (0, 1):
                p = own_plane[f]
                to_near = g_v[f, here, :] + 0.5 * rx_v[f, 1, j, at, :]
                to_far = rx_v[f, 2, j, at, :] + 0.5 * k_v[p, inner, :]
                step = rx_v[f, 0, j, at, :] - e_v[p, inner, :]
                push = to_far * step
                d_v[f, j, at, :] = -push
                here_half = h_v[p, inner, :] + to_near * step
                far_half = rx_v[f, 3, j, at, :] - push
                h_v[p, inner, :] = here_half
                step = far_half - here_half
                near_v[f, j, at, :] = to_near * step
                fix = -(to_far * step)
                far_v[f, j, at, :] = fix
                sums.append(carry[f] + folded(fix))
            return tuple(sums)

        spill = lax.fori_loop(0, tiles, body, spill)
        for f in (1, 0):
            copy = send(d_v.at[f, j], c_v.at[1 - f, j], s2.at[f, j], r2.at[1 - f, j], neighbour[f])
            copy.start()
            second.append(copy)

    def fix_copies(act):
        for j in range(halves):
            for f in (0, 1):
                far_place, far_block = lax.rem(side_slab[f], peers), lax.div(side_slab[f], peers)
                slot = lax.div(far_place, 2)
                for c in range(gy_n):
                    at_home = (mine[j] == gx) & (gy == c) & (far_block == gz)
                    act(
                        at_home, far_v.at[f, j, :, lanes(c)], corr.at[slot, 1 - f], sc.at[f, j, c],
                        rc.at[slot, 1 - f], {"gx": mine[j], "gy": jnp.int32(c), "gz": far_block},
                    )

    def begin(at_home, src, dst, send_sem, recv_sem, target):
        @pl.when(at_home)
        def _():
            pltpu.make_async_copy(src, dst, recv_sem).start()

        @pl.when(jnp.logical_not(at_home))
        def _():
            send(src, dst, send_sem, recv_sem, target).start()

    def finish(at_home, src, dst, send_sem, recv_sem, target):
        @pl.when(jnp.logical_not(at_home))
        def _():
            send(src, dst, send_sem, recv_sem, target).wait_send()

    fix_copies(begin)

    sums = [zero] * planes

    def second_step(block, j, own):
        for p in range(planes):

            def body(t, carry, p=p):
                start = pl.multiple_of(block * height + t * ROWS, 8)
                at = pl.ds(pl.multiple_of(t * ROWS, 8), ROWS)
                here, inner, value, half, speed = local(h_v, p, start)
                for f in (0, 1):
                    if own and p == own_plane[f]:
                        value = value + near_v[f, j, at, :]
                n_v[p, here, :] = value
                return carry + folded(value)

            sums[p] = lax.fori_loop(0, tiles, body, sums[p])

    def hand_out(block, j, own, act):
        for c in range(gy_n):
            at_home = (block == gx) & (gy == c)
            act(
                at_home, n_v.at[:, pl.ds(row(block), height), lanes(c)], out.at[pl.ds(place * planes, planes)],
                s3.at[2 * j + own, c], r3.at[place], {"gx": block, "gy": jnp.int32(c), "gz": gz},
            )

    for j in range(halves):
        for f in (0, 1):
            first[f, 3, j].wait_send()
            send(d_v.at[f, j], c_v.at[f, j], s2.at[f, j], r2.at[f, j], neighbour[f]).wait_recv()

        @pl.loop(0, tiles)
        def _(t, j=j):
            at = pl.ds(pl.multiple_of(t * ROWS, 8), ROWS)
            inner = pl.ds(pl.multiple_of(theirs[j] * height + t * ROWS + PAD, 8), ROWS)
            for f in (0, 1):
                h_v[own_plane[f], inner, :] = h_v[own_plane[f], inner, :] + c_v[f, j, at, :]

        second_step(theirs[j], j, 0)
        hand_out(theirs[j], j, 0, begin)
    for j in range(halves):
        second_step(mine[j], j, 1)
        hand_out(mine[j], j, 1, begin)

    spot = lax.broadcasted_iota(jnp.int32, (8, 128), 1)
    scale = 1.0 / (nx * ny)
    part = jnp.zeros((8, 128), jnp.float32)
    base = place * planes
    amounts = [jnp.sum(spill[0], keepdims=True)] + [jnp.sum(s, keepdims=True) for s in sums]
    amounts.append(jnp.sum(spill[1], keepdims=True))
    for i, amount in enumerate(amounts):
        part = jnp.where(spot == base + i, amount * scale, part)
    group_v[0] = part
    share = []
    for i in range(1, peers):
        copy = send(group_v.at[0], group_v.at[i], s4.at[i], r4.at[i], peer(i))
        copy.start()
        share.append(copy)
    for copy in share:
        copy.wait_recv()
    for i in range(1, peers):
        part = part + group_v[i]
    block_v[0] = part
    climb = []
    for i in range(1, gz_n):
        copy = send(block_v.at[0], block_v.at[i], s5.at[i], r5.at[i], layer(i))
        copy.start()
        climb.append(copy)
    for copy in climb:
        copy.wait_recv()
    lower = jnp.zeros((8, 128), jnp.float32)
    own_lane = (spot >= 1) & (spot <= count)
    means = jnp.where(own_lane, part, 0.0)
    for i in range(gz_n):
        vector = block_v[i]
        block = lax.rem(gz + gz_n - i, gz_n)
        owner = jnp.where(own_lane, block, jnp.where(
            spot == 0, lax.rem(block + gz_n - 1, gz_n), lax.rem(block + 1, gz_n)))
        vector = jnp.where(spot <= count + 1, vector, 0.0)
        lower = lower + jnp.where(owner < gz, vector, 0.0)
        low = jnp.sum(jnp.where((spot == 0) & (owner == gz), vector, 0.0)[0:1], axis=1, keepdims=True)
        high = jnp.sum(jnp.where((spot == count + 1) & (owner == gz), vector, 0.0)[0:1], axis=1, keepdims=True)
        means = means + jnp.where(spot == count, low, 0.0) + jnp.where(spot == 1, high, 0.0)
    means = pltpu.roll(means, 127, 1)
    running = means
    step = 1
    while step < count:
        running = running + jnp.where(spot >= step, pltpu.roll(running, step, 1), 0.0)
        step *= 2
    mean_ref[...] = means
    offset = jnp.sum(lower[0:1], axis=1, keepdims=True)
    rank = (gz * count + spot + 1).astype(jnp.float32)
    run_ref[...] = (running + offset) / rank

    for s in range(peers):
        dst = out.at[pl.ds(s * planes, planes)]
        send(dst, dst, s3.at[0, 0], r3.at[s], neighbour[0]).wait_recv()
    for slot in range(peers // 2):
        for f in (0, 1):
            send(corr.at[slot, f], corr.at[slot, f], sc.at[0, 0, 0], rc.at[slot, f], neighbour[0]).wait_recv()
    for j in range(halves):
        hand_out(theirs[j], j, 0, finish)
        hand_out(mine[j], j, 1, finish)
    fix_copies(finish)
    for key, copy in first.items():
        if key[1] != 3:
            copy.wait_send()
    for copy in second + share + climb:
        copy.wait_send()


def finish_kernel(planes, base_ref, corr_ref, mean_in, run_in, out_ref, mean_ref, run_ref):
    out_ref[...] = base_ref[...]
    start = (1 - lax.rem(lax.axis_index("gx"), 2)) * planes
    for f, p in ((0, 0), (1, planes - 1)):
        out_ref[start + p] = out_ref[start + p] + corr_ref[0, f]
    count = mean_ref.shape[0]
    mean_ref[...] = mean_in[0, 0:count]
    run_ref[...] = run_in[0, 0:count]


def by_parity(energy, flow):
    gx_n, gy_n, gz_n = (lax.axis_size(a) for a in ("gx", "gy", "gz"))
    planes, nx, ny = energy.shape
    peers, halves = gx_n * gy_n, gx_n // 2
    height, width = nx // gx_n, ny // gy_n
    dma = pltpu.SemaphoreType.DMA
    f32 = jnp.float32
    anywhere = pl.BlockSpec(memory_space=pl.ANY)
    vmem = pl.BlockSpec(memory_space=pltpu.VMEM)
    tall = pltpu.VMEM((planes, nx + 2 * PAD, ny), f32)
    faces = pltpu.VMEM((2, halves, height, ny), f32)
    base, corr, means, running = pl.pallas_call(
        functools.partial(split_kernel, (gx_n, gy_n, gz_n, planes, nx, ny)),
        out_shape=(
            jax.ShapeDtypeStruct((planes * peers, height, width), f32),
            jax.ShapeDtypeStruct((peers // 2, 2, height, width), f32),
            jax.ShapeDtypeStruct((8, 128), f32),
            jax.ShapeDtypeStruct((8, 128), f32),
        ),
        in_specs=[anywhere, anywhere],
        out_specs=(anywhere, anywhere, vmem, vmem),
        scratch_shapes=[
            tall, tall, pltpu.VMEM((3, planes, nx, ny), f32), tall,
            pltpu.VMEM((planes, nx, ny), f32), pltpu.VMEM((2, nx, ny), f32),
            pltpu.VMEM((2, 4, halves, height, ny), f32), faces, faces, faces, faces,
            pltpu.VMEM((peers, 8, 128), f32), pltpu.VMEM((gz_n, 8, 128), f32),
            dma((3,)), dma((2, 4, halves)), dma((2, 4, halves)), dma((2, halves)), dma((2, halves)),
            dma((gx_n, gy_n)), dma((peers,)), dma((2, halves, gy_n)), dma((peers // 2, 2)),
            dma((peers,)), dma((peers,)), dma((gz_n,)), dma((gz_n,)),
        ],
        compiler_params=pltpu.CompilerParams(collective_id=0, has_side_effects=True),
    )(energy, flow)
    steps, count = peers // 2, planes * peers
    row = pl.BlockSpec((8, 128), lambda i: (0, 0))
    line = pl.BlockSpec((count,), lambda i: (0,))
    return tuple(pl.pallas_call(
        functools.partial(finish_kernel, planes),
        grid=(steps,),
        out_shape=(
            jax.ShapeDtypeStruct((count, height, width), f32),
            jax.ShapeDtypeStruct((count,), f32),
            jax.ShapeDtypeStruct((count,), f32),
        ),
        in_specs=[
            pl.BlockSpec((2 * planes, height, width), lambda i: (i, 0, 0)),
            pl.BlockSpec((1, 2, height, width), lambda i: (i, 0, 0, 0)),
            row, row,
        ],
        out_specs=(pl.BlockSpec((2 * planes, height, width), lambda i: (i, 0, 0)), line, line),
    )(base, corr, means, running))


def per_device(energy, flow):
    gx_n, gy_n, gz_n = (lax.axis_size(a) for a in ("gx", "gy", "gz"))
    planes, nx, ny = energy.shape
    if planes > 1 and gx_n % 2 == 0 and gz_n > 1:
        return by_parity(energy, flow)
    peers = gx_n * gy_n
    parts = (1 if planes > 2 else 0) + (2 if planes > 1 else 1)
    dma = pltpu.SemaphoreType.DMA
    f32 = jnp.float32
    anywhere = pl.BlockSpec(memory_space=pl.ANY)
    vmem = pl.BlockSpec(memory_space=pltpu.VMEM)
    tall = pltpu.VMEM((planes + 2, nx + 2 * PAD, ny), f32)
    energy_next, means, running = pl.pallas_call(
        functools.partial(kernel, (gx_n, gy_n, gz_n, planes, nx, ny)),
        out_shape=(
            jax.ShapeDtypeStruct((planes * peers, nx // gx_n, ny // gy_n), f32),
            jax.ShapeDtypeStruct((8, 128), f32),
            jax.ShapeDtypeStruct((8, 128), f32),
        ),
        in_specs=[anywhere, anywhere],
        out_specs=(anywhere, vmem, vmem),
        scratch_shapes=[
            tall, tall, pltpu.VMEM((3, planes, nx, ny), f32), tall,
            pltpu.VMEM((planes, nx, ny), f32),
            pltpu.VMEM((peers, 8, 128), f32), pltpu.VMEM((gz_n, 8, 128), f32),
            dma((3,)), dma((gy_n, 4)), dma((gy_n, 4)), dma((gy_n, 2)), dma((gy_n, 2)),
            dma((peers, parts)), dma((peers, parts)), dma((parts,)),
            dma((peers,)), dma((peers,)), dma((gz_n,)), dma((gz_n,)),
        ],
        compiler_params=pltpu.CompilerParams(collective_id=0, has_side_effects=True),
    )(energy, flow)
    count = planes * peers
    return energy_next, means[0, :count], running[0, :count]


def solution(mesh):
    placed = (P(("gz", "gy", "gx"), None, None), P(None, ("gz", "gy", "gx"), None, None))
    return jax.shard_map(
        per_device,
        mesh=mesh,
        in_specs=placed,
        out_specs=(P("gz", "gx", "gy"), P("gz"), P("gz")),
        check_vma=False,
    )
```

```python
import functools

import jax
import jax.numpy as jnp
from jax import lax
from jax.experimental import pallas as pl
from jax.experimental.pallas import tpu as pltpu
from jax.sharding import PartitionSpec as P

MESH = pl.DeviceIdType.MESH
PAD = 8
ROWS = 16
STRIP = 32


def shifted(block, rows):
    size = block.shape[0]
    return (
        block[PAD : PAD + rows],
        pltpu.roll(block, size - 1, 0)[PAD : PAD + rows],
        pltpu.roll(block, 1, 0)[PAD : PAD + rows],
    )


def sideways(block, lane):
    width = block.shape[1]
    right = jnp.where(lane == width - 1, 0.0, pltpu.roll(block, width - 1, 1))
    left = jnp.where(lane == 0, 0.0, pltpu.roll(block, 1, 1))
    return right, left


def above(k, k_up, speed, e, e_up):
    return (0.5 * (k + k_up) - jnp.minimum(speed, 0.0)) * (e_up - e)


def below(k, k_down, speed, e, e_down):
    return (0.5 * (k + k_down) + jnp.maximum(speed, 0.0)) * (e_down - e)


def kernel(
    sizes, e_hbm, f_hbm, out, mean_ref, run_ref,
    e_v, k_v, u_v, h_v, n_v, group_v, block_v,
    load_sem, s1, r1, s2, r2, s3, r3, own_sem, s4, r4, s5, r5,
):
    gx_n, gy_n, gz_n, planes, nx, ny = sizes
    height, width = nx // gx_n, ny // gy_n
    gx, gy, gz = lax.axis_index("gx"), lax.axis_index("gy"), lax.axis_index("gz")
    peers = gx_n * gy_n
    place = gy * gx_n + gx
    slab = gz * peers + place

    def device(number):
        return {
            "gx": lax.rem(number, gx_n),
            "gy": lax.rem(lax.div(number, gx_n), gy_n),
            "gz": lax.div(number, peers),
        }

    total = peers * gz_n
    up = device(lax.rem(slab + 1, total))
    down = device(lax.rem(slab + total - 1, total))

    def peer(step):
        return {
            "gx": lax.rem(place + step, gx_n) if gy_n == 1 else lax.rem(lax.rem(place + step, peers), gx_n),
            "gy": lax.div(lax.rem(place + step, peers), gx_n),
            "gz": gz,
        }

    def layer(step):
        return {"gx": gx, "gy": gy, "gz": lax.rem(gz + step, gz_n)}

    loads = [
        pltpu.make_async_copy(e_hbm, e_v.at[pl.ds(1, planes), pl.ds(PAD, nx)], load_sem.at[0]),
        pltpu.make_async_copy(f_hbm.at[3], k_v.at[pl.ds(1, planes), pl.ds(PAD, nx)], load_sem.at[1]),
        pltpu.make_async_copy(f_hbm.at[pl.ds(0, 3)], u_v, load_sem.at[2]),
    ]

    barrier = pltpu.get_barrier_semaphore()
    greet = [up, down] + [peer(i) for i in range(1, peers)] + [layer(i) for i in range(1, gz_n)]
    for target in greet:
        pl.semaphore_signal(barrier, inc=1, device_id=target, device_id_type=MESH)
    for load in loads:
        load.start()
    edge = jnp.zeros((planes, PAD, ny), jnp.float32)
    for ref in (e_v, k_v, h_v):
        ref[1 : planes + 1, 0:PAD, :] = edge
        ref[1 : planes + 1, PAD + nx : PAD + nx + PAD, :] = edge
    pl.semaphore_wait(barrier, len(greet))

    def lanes(c):
        return pl.ds(c * width, width)

    def send(src, dst, send_sem, recv_sem, target):
        return pltpu.make_async_remote_copy(
            src_ref=src, dst_ref=dst, send_sem=send_sem, recv_sem=recv_sem,
            device_id=target, device_id_type=MESH,
        )

    first = []
    rows_all = pl.ds(PAD, nx)
    for c in range(gy_n):
        copies = [
            send(e_hbm.at[planes - 1, :, lanes(c)], e_v.at[0, rows_all, lanes(c)], s1.at[c, 0], r1.at[c, 0], up),
            send(e_hbm.at[0, :, lanes(c)], e_v.at[planes + 1, rows_all, lanes(c)], s1.at[c, 1], r1.at[c, 1], down),
            send(f_hbm.at[3, planes - 1, :, lanes(c)], k_v.at[0, rows_all, lanes(c)], s1.at[c, 2], r1.at[c, 2], up),
            send(f_hbm.at[3, 0, :, lanes(c)], k_v.at[planes + 1, rows_all, lanes(c)], s1.at[c, 3], r1.at[c, 3], down),
        ]
        for copy in copies:
            copy.start()
        first.append(copies)

    for load in loads:
        load.wait()

    lane = lax.broadcasted_iota(jnp.int32, (ROWS, ny), 1)

    def local(src, p, r):
        start = pl.multiple_of(r * ROWS, ROWS)
        here = pl.ds(start, ROWS)
        inner = pl.ds(pl.multiple_of(start + PAD, PAD), ROWS)
        tall = pl.ds(start, ROWS + 2 * PAD)
        e, e_next, e_prev = shifted(src[p + 1, tall, :], ROWS)
        k, k_next, k_prev = shifted(k_v[p + 1, tall, :], ROWS)
        speed = u_v[1, p, here, :]
        value = e + above(k, k_next, speed, e, e_next) + below(k, k_prev, speed, e, e_prev)
        e_next, e_prev = sideways(e, lane)
        k_next, k_prev = sideways(k, lane)
        speed = u_v[2, p, here, :]
        value = value + above(k, k_next, speed, e, e_next) + below(k, k_prev, speed, e, e_prev)
        speed = u_v[0, p, here, :]
        if p < planes - 1:
            value = value + above(k, k_v[p + 2, inner, :], speed, e, src[p + 2, inner, :])
        if p > 0:
            value = value + below(k, k_v[p, inner, :], speed, e, src[p, inner, :])
        return here, inner, value

    def edge_terms(src, c, r):
        start = pl.multiple_of(r * STRIP, STRIP)
        here = pl.ds(start, STRIP)
        inner = pl.ds(pl.multiple_of(start + PAD, PAD), STRIP)
        at = lanes(c)
        top = above(
            k_v[planes, inner, at], k_v[planes + 1, inner, at], u_v[0, planes - 1, here, at],
            src[planes, inner, at], src[planes + 1, inner, at],
        )
        bottom = below(
            k_v[1, inner, at], k_v[0, inner, at], u_v[0, 0, here, at], src[1, inner, at], src[0, inner, at]
        )
        return here, inner, top, bottom

    def folded(value):
        rows = value.shape[0]
        part = value[0:8]
        for i in range(8, rows, 8):
            part = part + value[i : i + 8]
        return part

    for p in range(planes):

        @pl.loop(0, nx // ROWS)
        def _(r, p=p):
            here, inner, value = local(e_v, p, r)
            h_v[p + 1, inner, :] = value

    second = []
    for c in range(gy_n):
        for copy in first[c]:
            copy.wait_recv()

        @pl.loop(0, nx // STRIP)
        def _(r, c=c):
            here, inner, top, bottom = edge_terms(e_v, c, r)
            h_v[planes, inner, lanes(c)] = h_v[planes, inner, lanes(c)] + top
            h_v[1, inner, lanes(c)] = h_v[1, inner, lanes(c)] + bottom

        copies = [
            send(h_v.at[planes, rows_all, lanes(c)], h_v.at[0, rows_all, lanes(c)], s2.at[c, 0], r2.at[c, 0], up),
            send(h_v.at[1, rows_all, lanes(c)], h_v.at[planes + 1, rows_all, lanes(c)], s2.at[c, 1], r2.at[c, 1], down),
        ]
        for copy in copies:
            copy.start()
        second.append(copies)

    sums = []
    for p in range(planes):

        def body(r, carry, p=p):
            here, inner, value = local(h_v, p, r)
            n_v[p, here, :] = value
            return carry + folded(value)

        sums.append(lax.fori_loop(0, nx // ROWS, body, jnp.zeros((8, ny), jnp.float32)))

    def hand_out(c, p0, count, part):
        for d in range(gx_n):
            to = lax.rem(gx + d, gx_n)
            src = n_v.at[pl.ds(p0, count), pl.ds(pl.multiple_of(to * height, 8), height), lanes(c)]
            dst = out.at[pl.ds(place * planes + p0, count)]
            if d == 0:

                @pl.when(gy == c)
                def _():
                    pltpu.make_async_copy(src, dst, own_sem.at[part]).start()

                @pl.when(gy != c)
                def _():
                    send(src, dst, s3.at[c * gx_n + d, part], r3.at[place, part],
                         {"gx": gx, "gy": jnp.int32(c), "gz": gz}).start()
            else:
                send(src, dst, s3.at[c * gx_n + d, part], r3.at[place, part],
                     {"gx": to, "gy": jnp.int32(c), "gz": gz}).start()

    parts = []
    if planes > 2:
        parts.append((1, planes - 2))
        for c in range(gy_n):
            hand_out(c, 1, planes - 2, 0)
    outer = sorted({0, planes - 1})
    first_outer = len(parts)
    parts += [(p, 1) for p in outer]

    extra = [jnp.zeros((8, width), jnp.float32), jnp.zeros((8, width), jnp.float32)]
    for c in range(gy_n):
        for copy in second[c]:
            copy.wait_recv()

        def body(r, carry, c=c):
            here, inner, top, bottom = edge_terms(h_v, c, r)
            n_v[planes - 1, here, lanes(c)] = n_v[planes - 1, here, lanes(c)] + top
            n_v[0, here, lanes(c)] = n_v[0, here, lanes(c)] + bottom
            return carry[0] + folded(top), carry[1] + folded(bottom)

        extra = lax.fori_loop(0, nx // STRIP, body, tuple(extra))
        for part, p in enumerate(outer):
            hand_out(c, p, 1, first_outer + part)

    spot = lax.broadcasted_iota(jnp.int32, (8, 128), 1)
    mine = jnp.zeros((8, 128), jnp.float32)
    for p in range(planes):
        amount = jnp.sum(sums[p], keepdims=True)
        if p == planes - 1:
            amount = amount + jnp.sum(extra[0], keepdims=True)
        if p == 0:
            amount = amount + jnp.sum(extra[1], keepdims=True)
        mine = jnp.where(spot == place * planes + p, amount * (1.0 / (nx * ny)), mine)
    group_v[0] = mine
    share = []
    for i in range(1, peers):
        copy = send(group_v.at[0], group_v.at[i], s4.at[i], r4.at[i], peer(i))
        copy.start()
        share.append(copy)
    for copy in share:
        copy.wait_recv()
    means = mine
    for i in range(1, peers):
        means = means + group_v[i]
    block_v[0] = means
    climb = []
    for i in range(1, gz_n):
        copy = send(block_v.at[0], block_v.at[i], s5.at[i], r5.at[i], layer(i))
        copy.start()
        climb.append(copy)
    running = means
    step = 1
    while step < peers * planes:
        running = running + jnp.where(spot >= step, pltpu.roll(running, step, 1), 0.0)
        step *= 2
    mean_ref[...] = means
    for copy in climb:
        copy.wait_recv()
    lower = jnp.zeros((8, 128), jnp.float32)
    for i in range(1, gz_n):
        lower = lower + jnp.where(gz >= i, block_v[i], 0.0)
    offset = jnp.sum(lower[0:1], axis=1, keepdims=True)
    rank = (gz * peers * planes + spot + 1).astype(jnp.float32)
    run_ref[...] = (running + offset) / rank

    for part, (p0, count) in enumerate(parts):
        for d in range(peers):
            source = lax.rem(place + d, peers)
            dst = out.at[pl.ds(source * planes + p0, count)]
            src = n_v.at[pl.ds(p0, count), pl.ds(0, height), pl.ds(0, width)]
            if d == 0:
                pltpu.make_async_copy(src, dst, own_sem.at[part]).wait()
            else:
                send(src, dst, s3.at[0, part], r3.at[source, part], peer(d)).wait_recv()
        for c in range(gy_n):
            for d in range(gx_n):
                copy = send(
                    n_v.at[pl.ds(p0, count), pl.ds(0, height), pl.ds(0, width)],
                    out.at[pl.ds(p0, count)], s3.at[c * gx_n + d, part], r3.at[0, part], up,
                )
                if d == 0:

                    @pl.when(gy != c)
                    def _():
                        copy.wait_send()
                else:
                    copy.wait_send()
    for copies in first + second + [share, climb]:
        for copy in copies:
            copy.wait_send()


def split_kernel(
    sizes, e_hbm, f_hbm, out, corr, mean_ref, run_ref,
    e_v, k_v, u_v, h_v, n_v, g_v, rx_v, d_v, c_v, near_v, far_v, group_v, block_v,
    load_sem, s1, r1, s2, r2, s3, r3, sc, rc, s4, r4, s5, r5,
):
    gx_n, gy_n, gz_n, planes, nx, ny = sizes
    height, width = nx // gx_n, ny // gy_n
    halves = gx_n // 2
    gx, gy, gz = lax.axis_index("gx"), lax.axis_index("gy"), lax.axis_index("gz")
    peers = gx_n * gy_n
    count = peers * planes
    place = gy * gx_n + gx
    slab = gz * peers + place
    parity = lax.rem(gx, 2)
    total = peers * gz_n
    above_slab, below_slab = lax.rem(slab + 1, total), lax.rem(slab + total - 1, total)
    last = planes - 1
    own_plane = (0, last)

    def device(number):
        return {
            "gx": lax.rem(number, gx_n),
            "gy": lax.rem(lax.div(number, gx_n), gy_n),
            "gz": lax.div(number, peers),
        }

    neighbour = (device(below_slab), device(above_slab))

    def peer(step):
        return device(gz * peers + lax.rem(place + step, peers))

    def layer(step):
        return {"gx": gx, "gy": gy, "gz": lax.rem(gz + step, gz_n)}

    loads = [
        pltpu.make_async_copy(e_hbm, e_v.at[:, pl.ds(PAD, nx)], load_sem.at[0]),
        pltpu.make_async_copy(f_hbm.at[3], k_v.at[:, pl.ds(PAD, nx)], load_sem.at[1]),
        pltpu.make_async_copy(f_hbm.at[pl.ds(0, 3)], u_v, load_sem.at[2]),
    ]
    for load in loads:
        load.start()

    barrier = pltpu.get_barrier_semaphore()
    greet = list(neighbour) + [peer(i) for i in range(1, peers)] + [layer(i) for i in range(1, gz_n)]
    greet.append(device(lax.rem(gz + gz_n - 1, gz_n) * peers + peers - 1))
    greet.append(device(lax.rem(gz + 1, gz_n) * peers))
    for target in greet:
        pl.semaphore_signal(barrier, inc=1, device_id=target, device_id_type=MESH)
    edge = jnp.zeros((planes, PAD, ny), jnp.float32)
    for ref in (e_v, k_v, h_v):
        ref[:, 0:PAD, :] = edge
        ref[:, PAD + nx : PAD + nx + PAD, :] = edge
    outermost = (place == 0).astype(jnp.int32) + (place == peers - 1).astype(jnp.int32)
    pl.semaphore_wait(barrier, len(greet) - 2 + outermost * peers)

    def lanes(c):
        return pl.ds(c * width, width)

    def send(src, dst, send_sem, recv_sem, target):
        return pltpu.make_async_remote_copy(
            src_ref=src, dst_ref=dst, send_sem=send_sem, recv_sem=recv_sem,
            device_id=target, device_id_type=MESH,
        )

    def row(block, extra=0):
        return pl.multiple_of(block * height + extra, 8)

    mine = [2 * j + parity for j in range(halves)]
    theirs = [2 * j + 1 - parity for j in range(halves)]

    first = {}

    def start_first(j, fields):
        for f in (1, 0):
            p, rows = own_plane[f], pl.ds(row(theirs[j]), height)
            inner = pl.ds(row(theirs[j], PAD), height)
            sources = (e_hbm.at[p, rows], f_hbm.at[3, p, rows], g_v.at[f, rows], h_v.at[p, inner])
            for i in fields:
                copy = send(sources[i], rx_v.at[1 - f, i, j], s1.at[f, i, j], r1.at[1 - f, i, j], neighbour[f])
                copy.start()
                first[f, i, j] = copy

    start_first(0, (0, 1))
    for load in loads:
        load.wait()

    lane = lax.broadcasted_iota(jnp.int32, (ROWS, ny), 1)
    tiles = height // ROWS

    def local(src, p, start):
        here = pl.ds(start, ROWS)
        inner = pl.ds(pl.multiple_of(start + PAD, 8), ROWS)
        tall = pl.ds(start, ROWS + 2 * PAD)
        e, e_next, e_prev = shifted(src[p, tall, :], ROWS)
        k, k_next, k_prev = shifted(k_v[p, tall, :], ROWS)
        speed = u_v[1, p, here, :]
        value = e + above(k, k_next, speed, e, e_next) + below(k, k_prev, speed, e, e_prev)
        e_next, e_prev = sideways(e, lane)
        k_next, k_prev = sideways(k, lane)
        speed = u_v[2, p, here, :]
        value = value + above(k, k_next, speed, e, e_next) + below(k, k_prev, speed, e, e_prev)
        speed = u_v[0, p, here, :]
        if p < last:
            value = value + above(k, k_v[p + 1, inner, :], speed, e, src[p + 1, inner, :])
        if p > 0:
            value = value + below(k, k_v[p - 1, inner, :], speed, e, src[p - 1, inner, :])
        return here, inner, value, 0.5 * k, speed

    def folded(value):
        part = value[0:8]
        for i in range(8, value.shape[0], 8):
            part = part + value[i : i + 8]
        return part

    def first_step(block, which):
        @pl.loop(0, tiles)
        def _(t):
            start = pl.multiple_of(block * height + t * ROWS, 8)
            for p in which:
                here, inner, value, half, speed = local(e_v, p, start)
                h_v[p, inner, :] = value
                if p == 0:
                    g_v[0, here, :] = half + jnp.maximum(speed, 0.0)
                if p == last:
                    g_v[1, here, :] = half - jnp.minimum(speed, 0.0)

    for j in range(halves):
        if j > 0:
            start_first(j, (0, 1))
        first_step(theirs[j], own_plane)
        start_first(j, (2, 3))
    for j in range(halves):
        first_step(mine[j], own_plane)
    inside = tuple(range(1, last))
    if inside:
        for block in range(gx_n):
            first_step(block, inside)

    second, fixes = [], []
    side_slab = (below_slab, above_slab)
    zero = jnp.zeros((8, ny), jnp.float32)
    spill = (zero, zero)
    for j in range(halves):
        for f in (0, 1):
            for i in range(4):
                send(rx_v.at[f, i, j], rx_v.at[f, i, j], s1.at[f, i, j], r1.at[f, i, j], neighbour[f]).wait_recv()

        def body(t, carry, j=j):
            sums = []
            at = pl.ds(pl.multiple_of(t * ROWS, 8), ROWS)
            start = pl.multiple_of(mine[j] * height + t * ROWS, 8)
            here, inner = pl.ds(start, ROWS), pl.ds(pl.multiple_of(start + PAD, 8), ROWS)
            for f in (0, 1):
                p = own_plane[f]
                to_near = g_v[f, here, :] + 0.5 * rx_v[f, 1, j, at, :]
                to_far = rx_v[f, 2, j, at, :] + 0.5 * k_v[p, inner, :]
                step = rx_v[f, 0, j, at, :] - e_v[p, inner, :]
                push = to_far * step
                d_v[f, j, at, :] = -push
                here_half = h_v[p, inner, :] + to_near * step
                far_half = rx_v[f, 3, j, at, :] - push
                h_v[p, inner, :] = here_half
                step = far_half - here_half
                near_v[f, j, at, :] = to_near * step
                fix = -(to_far * step)
                far_v[f, j, at, :] = fix
                sums.append(carry[f] + folded(fix))
            return tuple(sums)

        spill = lax.fori_loop(0, tiles, body, spill)
        for f in (1, 0):
            copy = send(d_v.at[f, j], c_v.at[1 - f, j], s2.at[f, j], r2.at[1 - f, j], neighbour[f])
            copy.start()
            second.append(copy)

    def fix_copies(act):
        for j in range(halves):
            for f in (0, 1):
                far_place, far_block = lax.rem(side_slab[f], peers), lax.div(side_slab[f], peers)
                slot = lax.div(far_place, 2)
                for c in range(gy_n):
                    at_home = (mine[j] == gx) & (gy == c) & (far_block == gz)
                    act(
                        at_home, far_v.at[f, j, :, lanes(c)], corr.at[slot, 1 - f], sc.at[f, j, c],
                        rc.at[slot, 1 - f], {"gx": mine[j], "gy": jnp.int32(c), "gz": far_block},
                    )

    def begin(at_home, src, dst, send_sem, recv_sem, target):
        @pl.when(at_home)
        def _():
            pltpu.make_async_copy(src, dst, recv_sem).start()

        @pl.when(jnp.logical_not(at_home))
        def _():
            send(src, dst, send_sem, recv_sem, target).start()

    def finish(at_home, src, dst, send_sem, recv_sem, target):
        @pl.when(jnp.logical_not(at_home))
        def _():
            send(src, dst, send_sem, recv_sem, target).wait_send()

    fix_copies(begin)

    sums = [zero] * planes

    def second_step(block, j, own):
        for p in range(planes):

            def body(t, carry, p=p):
                start = pl.multiple_of(block * height + t * ROWS, 8)
                at = pl.ds(pl.multiple_of(t * ROWS, 8), ROWS)
                here, inner, value, half, speed = local(h_v, p, start)
                for f in (0, 1):
                    if own and p == own_plane[f]:
                        value = value + near_v[f, j, at, :]
                n_v[p, here, :] = value
                return carry + folded(value)

            sums[p] = lax.fori_loop(0, tiles, body, sums[p])

    def hand_out(block, j, own, act):
        for c in range(gy_n):
            at_home = (block == gx) & (gy == c)
            act(
                at_home, n_v.at[:, pl.ds(row(block), height), lanes(c)], out.at[pl.ds(place * planes, planes)],
                s3.at[2 * j + own, c], r3.at[place], {"gx": block, "gy": jnp.int32(c), "gz": gz},
            )

    for j in range(halves):
        for f in (0, 1):
            first[f, 3, j].wait_send()
            send(d_v.at[f, j], c_v.at[f, j], s2.at[f, j], r2.at[f, j], neighbour[f]).wait_recv()

        @pl.loop(0, tiles)
        def _(t, j=j):
            at = pl.ds(pl.multiple_of(t * ROWS, 8), ROWS)
            inner = pl.ds(pl.multiple_of(theirs[j] * height + t * ROWS + PAD, 8), ROWS)
            for f in (0, 1):
                h_v[own_plane[f], inner, :] = h_v[own_plane[f], inner, :] + c_v[f, j, at, :]

        second_step(theirs[j], j, 0)
        if j < halves - 1:
            hand_out(theirs[j], j, 0, begin)
    for j in range(halves):
        second_step(mine[j], j, 1)

    spot = lax.broadcasted_iota(jnp.int32, (8, 128), 1)
    scale = 1.0 / (nx * ny)
    part = jnp.zeros((8, 128), jnp.float32)
    base = place * planes
    amounts = [jnp.sum(spill[0], keepdims=True)] + [jnp.sum(s, keepdims=True) for s in sums]
    amounts.append(jnp.sum(spill[1], keepdims=True))
    for i, amount in enumerate(amounts):
        part = jnp.where(spot == base + i, amount * scale, part)
    group_v[0] = part
    share = []
    for i in range(1, peers):
        copy = send(group_v.at[0], group_v.at[i], s4.at[i], r4.at[i], peer(i))
        copy.start()
        share.append(copy)
    hand_out(theirs[-1], halves - 1, 0, begin)
    for j in range(halves):
        hand_out(mine[j], j, 1, begin)
    for copy in share:
        copy.wait_recv()
    for i in range(1, peers):
        part = part + group_v[i]
    block_v[0] = part
    climb = []
    for i in range(1, gz_n):
        copy = send(block_v.at[0], block_v.at[i], s5.at[i], r5.at[i], layer(i))
        copy.start()
        climb.append(copy)
    for copy in climb:
        copy.wait_recv()
    lower = jnp.zeros((8, 128), jnp.float32)
    own_lane = (spot >= 1) & (spot <= count)
    means = jnp.where(own_lane, part, 0.0)
    for i in range(gz_n):
        vector = block_v[i]
        block = lax.rem(gz + gz_n - i, gz_n)
        owner = jnp.where(own_lane, block, jnp.where(
            spot == 0, lax.rem(block + gz_n - 1, gz_n), lax.rem(block + 1, gz_n)))
        vector = jnp.where(spot <= count + 1, vector, 0.0)
        lower = lower + jnp.where(owner < gz, vector, 0.0)
        low = jnp.sum(jnp.where((spot == 0) & (owner == gz), vector, 0.0)[0:1], axis=1, keepdims=True)
        high = jnp.sum(jnp.where((spot == count + 1) & (owner == gz), vector, 0.0)[0:1], axis=1, keepdims=True)
        means = means + jnp.where(spot == count, low, 0.0) + jnp.where(spot == 1, high, 0.0)
    means = pltpu.roll(means, 127, 1)
    running = means
    step = 1
    while step < count:
        running = running + jnp.where(spot >= step, pltpu.roll(running, step, 1), 0.0)
        step *= 2
    mean_ref[...] = means
    offset = jnp.sum(lower[0:1], axis=1, keepdims=True)
    rank = (gz * count + spot + 1).astype(jnp.float32)
    run_ref[...] = (running + offset) / rank

    for s in range(peers):
        dst = out.at[pl.ds(s * planes, planes)]
        send(dst, dst, s3.at[0, 0], r3.at[s], neighbour[0]).wait_recv()
    for slot in range(peers // 2):
        for f in (0, 1):
            send(corr.at[slot, f], corr.at[slot, f], sc.at[0, 0, 0], rc.at[slot, f], neighbour[0]).wait_recv()
    for j in range(halves):
        hand_out(theirs[j], j, 0, finish)
        hand_out(mine[j], j, 1, finish)
    fix_copies(finish)
    for key, copy in first.items():
        if key[1] != 3:
            copy.wait_send()
    for copy in second + share + climb:
        copy.wait_send()


def finish_kernel(planes, base_ref, corr_ref, mean_in, run_in, out_ref, mean_ref, run_ref, fix_v, done):
    other = 1 - lax.rem(lax.axis_index("gx"), 2)
    copies = []
    for slot in range(corr_ref.shape[0]):
        whole = pl.ds((2 * slot + 1 - other) * planes, planes)
        copies.append(pltpu.make_async_copy(base_ref.at[whole], out_ref.at[whole], done.at[slot, 0]))
        copies[-1].start()
    for slot in range(corr_ref.shape[0]):
        start = (2 * slot + other) * planes
        fix_v[slot] = base_ref[pl.ds(start, planes)]
        for f, p in ((0, 0), (1, planes - 1)):
            fix_v[slot, p] = fix_v[slot, p] + corr_ref[slot, f]
        copies.append(pltpu.make_async_copy(fix_v.at[slot], out_ref.at[pl.ds(start, planes)], done.at[slot, 1]))
        copies[-1].start()
    count = mean_ref.shape[0]
    mean_ref[...] = mean_in[0, 0:count]
    run_ref[...] = run_in[0, 0:count]
    for copy in copies:
        copy.wait()


def by_parity(energy, flow):
    gx_n, gy_n, gz_n = (lax.axis_size(a) for a in ("gx", "gy", "gz"))
    planes, nx, ny = energy.shape
    peers, halves = gx_n * gy_n, gx_n // 2
    height, width = nx // gx_n, ny // gy_n
    dma = pltpu.SemaphoreType.DMA
    f32 = jnp.float32
    anywhere = pl.BlockSpec(memory_space=pl.ANY)
    vmem = pl.BlockSpec(memory_space=pltpu.VMEM)
    tall = pltpu.VMEM((planes, nx + 2 * PAD, ny), f32)
    hbm = pl.BlockSpec(memory_space=pltpu.HBM)
    faces = pltpu.VMEM((2, halves, height, ny), f32)
    energy, flow = (pltpu.with_memory_space_constraint(x, pltpu.HBM) for x in (energy, flow))
    base, corr, means, running = pl.pallas_call(
        functools.partial(split_kernel, (gx_n, gy_n, gz_n, planes, nx, ny)),
        out_shape=(
            jax.ShapeDtypeStruct((planes * peers, height, width), f32),
            jax.ShapeDtypeStruct((peers // 2, 2, height, width), f32),
            jax.ShapeDtypeStruct((8, 128), f32),
            jax.ShapeDtypeStruct((8, 128), f32),
        ),
        in_specs=[hbm, hbm],
        out_specs=(anywhere, anywhere, vmem, vmem),
        scratch_shapes=[
            tall, tall, pltpu.VMEM((3, planes, nx, ny), f32), tall,
            pltpu.VMEM((planes, nx, ny), f32), pltpu.VMEM((2, nx, ny), f32),
            pltpu.VMEM((2, 4, halves, height, ny), f32), faces, faces, faces, faces,
            pltpu.VMEM((peers, 8, 128), f32), pltpu.VMEM((gz_n, 8, 128), f32),
            dma((3,)), dma((2, 4, halves)), dma((2, 4, halves)), dma((2, halves)), dma((2, halves)),
            dma((gx_n, gy_n)), dma((peers,)), dma((2, halves, gy_n)), dma((peers // 2, 2)),
            dma((peers,)), dma((peers,)), dma((gz_n,)), dma((gz_n,)),
        ],
        compiler_params=pltpu.CompilerParams(
            collective_id=0, has_side_effects=True, vmem_limit_bytes=8 * (energy.size + flow.size)
        ),
    )(energy, flow)
    count = planes * peers
    return tuple(pl.pallas_call(
        functools.partial(finish_kernel, planes),
        out_shape=(
            jax.ShapeDtypeStruct((count, height, width), f32),
            jax.ShapeDtypeStruct((count,), f32),
            jax.ShapeDtypeStruct((count,), f32),
        ),
        in_specs=[vmem] * 4,
        out_specs=(pl.BlockSpec(memory_space=pltpu.HBM), vmem, vmem),
        scratch_shapes=[pltpu.VMEM((peers // 2, planes, height, width), f32), dma((peers // 2, 2))],
        compiler_params=pltpu.CompilerParams(vmem_limit_bytes=8 * (energy.size + flow.size)),
    )(base, corr, means, running))


def per_device(energy, flow):
    gx_n, gy_n, gz_n = (lax.axis_size(a) for a in ("gx", "gy", "gz"))
    planes, nx, ny = energy.shape
    if planes > 1 and gx_n % 2 == 0 and gz_n > 1:
        return by_parity(energy, flow)
    peers = gx_n * gy_n
    parts = (1 if planes > 2 else 0) + (2 if planes > 1 else 1)
    dma = pltpu.SemaphoreType.DMA
    f32 = jnp.float32
    anywhere = pl.BlockSpec(memory_space=pl.ANY)
    vmem = pl.BlockSpec(memory_space=pltpu.VMEM)
    tall = pltpu.VMEM((planes + 2, nx + 2 * PAD, ny), f32)
    energy_next, means, running = pl.pallas_call(
        functools.partial(kernel, (gx_n, gy_n, gz_n, planes, nx, ny)),
        out_shape=(
            jax.ShapeDtypeStruct((planes * peers, nx // gx_n, ny // gy_n), f32),
            jax.ShapeDtypeStruct((8, 128), f32),
            jax.ShapeDtypeStruct((8, 128), f32),
        ),
        in_specs=[anywhere, anywhere],
        out_specs=(anywhere, vmem, vmem),
        scratch_shapes=[
            tall, tall, pltpu.VMEM((3, planes, nx, ny), f32), tall,
            pltpu.VMEM((planes, nx, ny), f32),
            pltpu.VMEM((peers, 8, 128), f32), pltpu.VMEM((gz_n, 8, 128), f32),
            dma((3,)), dma((gy_n, 4)), dma((gy_n, 4)), dma((gy_n, 2)), dma((gy_n, 2)),
            dma((peers, parts)), dma((peers, parts)), dma((parts,)),
            dma((peers,)), dma((peers,)), dma((gz_n,)), dma((gz_n,)),
        ],
        compiler_params=pltpu.CompilerParams(collective_id=0, has_side_effects=True),
    )(energy, flow)
    count = planes * peers
    return energy_next, means[0, :count], running[0, :count]


def solution(mesh):
    placed = (P(("gz", "gy", "gx"), None, None), P(None, ("gz", "gy", "gx"), None, None))
    return jax.shard_map(
        per_device,
        mesh=mesh,
        in_specs=placed,
        out_specs=(P("gz", "gx", "gy"), P("gz"), P("gz")),
        check_vma=False,
    )
```

```python
import functools

import jax
import jax.numpy as jnp
from jax import lax
from jax.experimental import pallas as pl
from jax.experimental.pallas import tpu as pltpu
from jax.sharding import PartitionSpec as P

MESH = pl.DeviceIdType.MESH
PAD = 8
ROWS = 16
STRIP = 32


def shifted(block, rows):
    size = block.shape[0]
    return (
        block[PAD : PAD + rows],
        pltpu.roll(block, size - 1, 0)[PAD : PAD + rows],
        pltpu.roll(block, 1, 0)[PAD : PAD + rows],
    )


def sideways(block, lane):
    width = block.shape[1]
    right = jnp.where(lane == width - 1, 0.0, pltpu.roll(block, width - 1, 1))
    left = jnp.where(lane == 0, 0.0, pltpu.roll(block, 1, 1))
    return right, left


def above(k, k_up, speed, e, e_up):
    return (0.5 * (k + k_up) - jnp.minimum(speed, 0.0)) * (e_up - e)


def below(k, k_down, speed, e, e_down):
    return (0.5 * (k + k_down) + jnp.maximum(speed, 0.0)) * (e_down - e)


def kernel(
    sizes, e_hbm, f_hbm, out, mean_ref, run_ref,
    e_v, k_v, u_v, h_v, n_v, group_v, block_v,
    load_sem, s1, r1, s2, r2, s3, r3, own_sem, s4, r4, s5, r5,
):
    gx_n, gy_n, gz_n, planes, nx, ny = sizes
    height, width = nx // gx_n, ny // gy_n
    gx, gy, gz = lax.axis_index("gx"), lax.axis_index("gy"), lax.axis_index("gz")
    peers = gx_n * gy_n
    place = gy * gx_n + gx
    slab = gz * peers + place

    def device(number):
        return {
            "gx": lax.rem(number, gx_n),
            "gy": lax.rem(lax.div(number, gx_n), gy_n),
            "gz": lax.div(number, peers),
        }

    total = peers * gz_n
    up = device(lax.rem(slab + 1, total))
    down = device(lax.rem(slab + total - 1, total))

    def peer(step):
        return {
            "gx": lax.rem(place + step, gx_n) if gy_n == 1 else lax.rem(lax.rem(place + step, peers), gx_n),
            "gy": lax.div(lax.rem(place + step, peers), gx_n),
            "gz": gz,
        }

    def layer(step):
        return {"gx": gx, "gy": gy, "gz": lax.rem(gz + step, gz_n)}

    loads = [
        pltpu.make_async_copy(e_hbm, e_v.at[pl.ds(1, planes), pl.ds(PAD, nx)], load_sem.at[0]),
        pltpu.make_async_copy(f_hbm.at[3], k_v.at[pl.ds(1, planes), pl.ds(PAD, nx)], load_sem.at[1]),
        pltpu.make_async_copy(f_hbm.at[pl.ds(0, 3)], u_v, load_sem.at[2]),
    ]

    barrier = pltpu.get_barrier_semaphore()
    greet = [up, down] + [peer(i) for i in range(1, peers)] + [layer(i) for i in range(1, gz_n)]
    for target in greet:
        pl.semaphore_signal(barrier, inc=1, device_id=target, device_id_type=MESH)
    for load in loads:
        load.start()
    edge = jnp.zeros((planes, PAD, ny), jnp.float32)
    for ref in (e_v, k_v, h_v):
        ref[1 : planes + 1, 0:PAD, :] = edge
        ref[1 : planes + 1, PAD + nx : PAD + nx + PAD, :] = edge
    pl.semaphore_wait(barrier, len(greet))

    def lanes(c):
        return pl.ds(c * width, width)

    def send(src, dst, send_sem, recv_sem, target):
        return pltpu.make_async_remote_copy(
            src_ref=src, dst_ref=dst, send_sem=send_sem, recv_sem=recv_sem,
            device_id=target, device_id_type=MESH,
        )

    first = []
    rows_all = pl.ds(PAD, nx)
    for c in range(gy_n):
        copies = [
            send(e_hbm.at[planes - 1, :, lanes(c)], e_v.at[0, rows_all, lanes(c)], s1.at[c, 0], r1.at[c, 0], up),
            send(e_hbm.at[0, :, lanes(c)], e_v.at[planes + 1, rows_all, lanes(c)], s1.at[c, 1], r1.at[c, 1], down),
            send(f_hbm.at[3, planes - 1, :, lanes(c)], k_v.at[0, rows_all, lanes(c)], s1.at[c, 2], r1.at[c, 2], up),
            send(f_hbm.at[3, 0, :, lanes(c)], k_v.at[planes + 1, rows_all, lanes(c)], s1.at[c, 3], r1.at[c, 3], down),
        ]
        for copy in copies:
            copy.start()
        first.append(copies)

    for load in loads:
        load.wait()

    lane = lax.broadcasted_iota(jnp.int32, (ROWS, ny), 1)

    def local(src, p, r):
        start = pl.multiple_of(r * ROWS, ROWS)
        here = pl.ds(start, ROWS)
        inner = pl.ds(pl.multiple_of(start + PAD, PAD), ROWS)
        tall = pl.ds(start, ROWS + 2 * PAD)
        e, e_next, e_prev = shifted(src[p + 1, tall, :], ROWS)
        k, k_next, k_prev = shifted(k_v[p + 1, tall, :], ROWS)
        speed = u_v[1, p, here, :]
        value = e + above(k, k_next, speed, e, e_next) + below(k, k_prev, speed, e, e_prev)
        e_next, e_prev = sideways(e, lane)
        k_next, k_prev = sideways(k, lane)
        speed = u_v[2, p, here, :]
        value = value + above(k, k_next, speed, e, e_next) + below(k, k_prev, speed, e, e_prev)
        speed = u_v[0, p, here, :]
        if p < planes - 1:
            value = value + above(k, k_v[p + 2, inner, :], speed, e, src[p + 2, inner, :])
        if p > 0:
            value = value + below(k, k_v[p, inner, :], speed, e, src[p, inner, :])
        return here, inner, value

    def edge_terms(src, c, r):
        start = pl.multiple_of(r * STRIP, STRIP)
        here = pl.ds(start, STRIP)
        inner = pl.ds(pl.multiple_of(start + PAD, PAD), STRIP)
        at = lanes(c)
        top = above(
            k_v[planes, inner, at], k_v[planes + 1, inner, at], u_v[0, planes - 1, here, at],
            src[planes, inner, at], src[planes + 1, inner, at],
        )
        bottom = below(
            k_v[1, inner, at], k_v[0, inner, at], u_v[0, 0, here, at], src[1, inner, at], src[0, inner, at]
        )
        return here, inner, top, bottom

    def folded(value):
        rows = value.shape[0]
        part = value[0:8]
        for i in range(8, rows, 8):
            part = part + value[i : i + 8]
        return part

    for p in range(planes):

        @pl.loop(0, nx // ROWS)
        def _(r, p=p):
            here, inner, value = local(e_v, p, r)
            h_v[p + 1, inner, :] = value

    second = []
    for c in range(gy_n):
        for copy in first[c]:
            copy.wait_recv()

        @pl.loop(0, nx // STRIP)
        def _(r, c=c):
            here, inner, top, bottom = edge_terms(e_v, c, r)
            h_v[planes, inner, lanes(c)] = h_v[planes, inner, lanes(c)] + top
            h_v[1, inner, lanes(c)] = h_v[1, inner, lanes(c)] + bottom

        copies = [
            send(h_v.at[planes, rows_all, lanes(c)], h_v.at[0, rows_all, lanes(c)], s2.at[c, 0], r2.at[c, 0], up),
            send(h_v.at[1, rows_all, lanes(c)], h_v.at[planes + 1, rows_all, lanes(c)], s2.at[c, 1], r2.at[c, 1], down),
        ]
        for copy in copies:
            copy.start()
        second.append(copies)

    sums = []
    for p in range(planes):

        def body(r, carry, p=p):
            here, inner, value = local(h_v, p, r)
            n_v[p, here, :] = value
            return carry + folded(value)

        sums.append(lax.fori_loop(0, nx // ROWS, body, jnp.zeros((8, ny), jnp.float32)))

    def hand_out(c, p0, count, part):
        for d in range(gx_n):
            to = lax.rem(gx + d, gx_n)
            src = n_v.at[pl.ds(p0, count), pl.ds(pl.multiple_of(to * height, 8), height), lanes(c)]
            dst = out.at[pl.ds(place * planes + p0, count)]
            if d == 0:

                @pl.when(gy == c)
                def _():
                    pltpu.make_async_copy(src, dst, own_sem.at[part]).start()

                @pl.when(gy != c)
                def _():
                    send(src, dst, s3.at[c * gx_n + d, part], r3.at[place, part],
                         {"gx": gx, "gy": jnp.int32(c), "gz": gz}).start()
            else:
                send(src, dst, s3.at[c * gx_n + d, part], r3.at[place, part],
                     {"gx": to, "gy": jnp.int32(c), "gz": gz}).start()

    parts = []
    if planes > 2:
        parts.append((1, planes - 2))
        for c in range(gy_n):
            hand_out(c, 1, planes - 2, 0)
    outer = sorted({0, planes - 1})
    first_outer = len(parts)
    parts += [(p, 1) for p in outer]

    extra = [jnp.zeros((8, width), jnp.float32), jnp.zeros((8, width), jnp.float32)]
    for c in range(gy_n):
        for copy in second[c]:
            copy.wait_recv()

        def body(r, carry, c=c):
            here, inner, top, bottom = edge_terms(h_v, c, r)
            n_v[planes - 1, here, lanes(c)] = n_v[planes - 1, here, lanes(c)] + top
            n_v[0, here, lanes(c)] = n_v[0, here, lanes(c)] + bottom
            return carry[0] + folded(top), carry[1] + folded(bottom)

        extra = lax.fori_loop(0, nx // STRIP, body, tuple(extra))
        for part, p in enumerate(outer):
            hand_out(c, p, 1, first_outer + part)

    spot = lax.broadcasted_iota(jnp.int32, (8, 128), 1)
    mine = jnp.zeros((8, 128), jnp.float32)
    for p in range(planes):
        amount = jnp.sum(sums[p], keepdims=True)
        if p == planes - 1:
            amount = amount + jnp.sum(extra[0], keepdims=True)
        if p == 0:
            amount = amount + jnp.sum(extra[1], keepdims=True)
        mine = jnp.where(spot == place * planes + p, amount * (1.0 / (nx * ny)), mine)
    group_v[0] = mine
    share = []
    for i in range(1, peers):
        copy = send(group_v.at[0], group_v.at[i], s4.at[i], r4.at[i], peer(i))
        copy.start()
        share.append(copy)
    for copy in share:
        copy.wait_recv()
    means = mine
    for i in range(1, peers):
        means = means + group_v[i]
    block_v[0] = means
    climb = []
    for i in range(1, gz_n):
        copy = send(block_v.at[0], block_v.at[i], s5.at[i], r5.at[i], layer(i))
        copy.start()
        climb.append(copy)
    running = means
    step = 1
    while step < peers * planes:
        running = running + jnp.where(spot >= step, pltpu.roll(running, step, 1), 0.0)
        step *= 2
    mean_ref[...] = means
    for copy in climb:
        copy.wait_recv()
    lower = jnp.zeros((8, 128), jnp.float32)
    for i in range(1, gz_n):
        lower = lower + jnp.where(gz >= i, block_v[i], 0.0)
    offset = jnp.sum(lower[0:1], axis=1, keepdims=True)
    rank = (gz * peers * planes + spot + 1).astype(jnp.float32)
    run_ref[...] = (running + offset) / rank

    for part, (p0, count) in enumerate(parts):
        for d in range(peers):
            source = lax.rem(place + d, peers)
            dst = out.at[pl.ds(source * planes + p0, count)]
            src = n_v.at[pl.ds(p0, count), pl.ds(0, height), pl.ds(0, width)]
            if d == 0:
                pltpu.make_async_copy(src, dst, own_sem.at[part]).wait()
            else:
                send(src, dst, s3.at[0, part], r3.at[source, part], peer(d)).wait_recv()
        for c in range(gy_n):
            for d in range(gx_n):
                copy = send(
                    n_v.at[pl.ds(p0, count), pl.ds(0, height), pl.ds(0, width)],
                    out.at[pl.ds(p0, count)], s3.at[c * gx_n + d, part], r3.at[0, part], up,
                )
                if d == 0:

                    @pl.when(gy != c)
                    def _():
                        copy.wait_send()
                else:
                    copy.wait_send()
    for copies in first + second + [share, climb]:
        for copy in copies:
            copy.wait_send()


def split_kernel(
    sizes, e_hbm, f_hbm, out, corr, mean_ref, run_ref,
    e_v, k_v, u_v, h_v, n_v, g_v, rx_v, d_v, c_v, near_v, far_v, group_v, block_v,
    load_sem, s1, r1, s2, r2, s3, r3, sc, rc, s4, r4, s5, r5,
):
    gx_n, gy_n, gz_n, planes, nx, ny = sizes
    height, width = nx // gx_n, ny // gy_n
    halves = gx_n // 2
    gx, gy, gz = lax.axis_index("gx"), lax.axis_index("gy"), lax.axis_index("gz")
    peers = gx_n * gy_n
    count = peers * planes
    place = gy * gx_n + gx
    slab = gz * peers + place
    parity = lax.rem(gx, 2)
    total = peers * gz_n
    above_slab, below_slab = lax.rem(slab + 1, total), lax.rem(slab + total - 1, total)
    last = planes - 1
    own_plane = (0, last)

    def device(number):
        return {
            "gx": lax.rem(number, gx_n),
            "gy": lax.rem(lax.div(number, gx_n), gy_n),
            "gz": lax.div(number, peers),
        }

    neighbour = (device(below_slab), device(above_slab))

    def peer(step):
        return device(gz * peers + lax.rem(place + step, peers))

    def layer(step):
        return {"gx": gx, "gy": gy, "gz": lax.rem(gz + step, gz_n)}

    loads = [
        pltpu.make_async_copy(e_hbm, e_v.at[:, pl.ds(PAD, nx)], load_sem.at[0]),
        pltpu.make_async_copy(f_hbm.at[3], k_v.at[:, pl.ds(PAD, nx)], load_sem.at[1]),
        pltpu.make_async_copy(f_hbm.at[pl.ds(0, 3)], u_v, load_sem.at[2]),
    ]
    for load in loads:
        load.start()

    barrier = pltpu.get_barrier_semaphore()
    greet = list(neighbour) + [peer(i) for i in range(1, peers)] + [layer(i) for i in range(1, gz_n)]
    greet.append(device(lax.rem(gz + gz_n - 1, gz_n) * peers + peers - 1))
    greet.append(device(lax.rem(gz + 1, gz_n) * peers))
    for target in greet:
        pl.semaphore_signal(barrier, inc=1, device_id=target, device_id_type=MESH)
    edge = jnp.zeros((planes, PAD, ny), jnp.float32)
    for ref in (e_v, k_v, h_v):
        ref[:, 0:PAD, :] = edge
        ref[:, PAD + nx : PAD + nx + PAD, :] = edge
    outermost = (place == 0).astype(jnp.int32) + (place == peers - 1).astype(jnp.int32)
    pl.semaphore_wait(barrier, len(greet) - 2 + outermost * peers)

    def lanes(c):
        return pl.ds(c * width, width)

    def send(src, dst, send_sem, recv_sem, target):
        return pltpu.make_async_remote_copy(
            src_ref=src, dst_ref=dst, send_sem=send_sem, recv_sem=recv_sem,
            device_id=target, device_id_type=MESH,
        )

    def row(block, extra=0):
        return pl.multiple_of(block * height + extra, 8)

    mine = [2 * j + parity for j in range(halves)]
    theirs = [2 * j + 1 - parity for j in range(halves)]

    first = {}

    def start_first(j, fields):
        for f in (1, 0):
            p, rows = own_plane[f], pl.ds(row(theirs[j]), height)
            inner = pl.ds(row(theirs[j], PAD), height)
            sources = (e_hbm.at[p, rows], f_hbm.at[3, p, rows], g_v.at[f, rows], h_v.at[p, inner])
            for i in fields:
                copy = send(sources[i], rx_v.at[1 - f, i, j], s1.at[f, i, j], r1.at[1 - f, i, j], neighbour[f])
                copy.start()
                first[f, i, j] = copy

    start_first(0, (0, 1))
    for load in loads:
        load.wait()

    lane = lax.broadcasted_iota(jnp.int32, (ROWS, ny), 1)
    tiles = height // ROWS

    def local(src, p, start):
        here = pl.ds(start, ROWS)
        inner = pl.ds(pl.multiple_of(start + PAD, 8), ROWS)
        tall = pl.ds(start, ROWS + 2 * PAD)
        e, e_next, e_prev = shifted(src[p, tall, :], ROWS)
        k, k_next, k_prev = shifted(k_v[p, tall, :], ROWS)
        speed = u_v[1, p, here, :]
        value = e + above(k, k_next, speed, e, e_next) + below(k, k_prev, speed, e, e_prev)
        e_next, e_prev = sideways(e, lane)
        k_next, k_prev = sideways(k, lane)
        speed = u_v[2, p, here, :]
        value = value + above(k, k_next, speed, e, e_next) + below(k, k_prev, speed, e, e_prev)
        speed = u_v[0, p, here, :]
        if p < last:
            value = value + above(k, k_v[p + 1, inner, :], speed, e, src[p + 1, inner, :])
        if p > 0:
            value = value + below(k, k_v[p - 1, inner, :], speed, e, src[p - 1, inner, :])
        return here, inner, value, 0.5 * k, speed

    def folded(value):
        part = value[0:8]
        for i in range(8, value.shape[0], 8):
            part = part + value[i : i + 8]
        return part

    def first_step(block, which):
        @pl.loop(0, tiles)
        def _(t):
            start = pl.multiple_of(block * height + t * ROWS, 8)
            for p in which:
                here, inner, value, half, speed = local(e_v, p, start)
                h_v[p, inner, :] = value
                if p == 0:
                    g_v[0, here, :] = half + jnp.maximum(speed, 0.0)
                if p == last:
                    g_v[1, here, :] = half - jnp.minimum(speed, 0.0)

    for j in range(halves):
        if j > 0:
            start_first(j, (0, 1))
        first_step(theirs[j], own_plane)
        start_first(j, (2, 3))
    for j in range(halves):
        first_step(mine[j], own_plane)
    inside = tuple(range(1, last))
    if inside:
        for block in range(gx_n):
            first_step(block, inside)

    second, fixes = [], []
    side_slab = (below_slab, above_slab)
    zero = jnp.zeros((8, ny), jnp.float32)
    spill = (zero, zero)
    sums = [zero] * planes

    def second_step(block, j, own, p, low, high):
        def body(t, carry):
            start = pl.multiple_of(block * height + t * ROWS, 8)
            at = pl.ds(pl.multiple_of(t * ROWS, 8), ROWS)
            here, inner, value, half, speed = local(h_v, p, start)
            for f in (0, 1):
                if own and p == own_plane[f]:
                    value = value + near_v[f, j, at, :]
            n_v[p, here, :] = value
            return carry + folded(value)

        sums[p] = lax.fori_loop(low, high, body, sums[p])

    def ahead(j):
        for p in range(planes):
            inside = 0 < p < last
            second_step(mine[j], j, 1, p, 0 if inside else 1, tiles if inside else tiles - 1)

    def behind(j):
        for p in own_plane:
            for t in sorted({0, tiles - 1}):
                second_step(mine[j], j, 1, p, t, t + 1)

    for j in range(halves):
        for f in (0, 1):
            for i in range(4):
                send(rx_v.at[f, i, j], rx_v.at[f, i, j], s1.at[f, i, j], r1.at[f, i, j], neighbour[f]).wait_recv()

        def body(t, carry, j=j):
            sums = []
            at = pl.ds(pl.multiple_of(t * ROWS, 8), ROWS)
            start = pl.multiple_of(mine[j] * height + t * ROWS, 8)
            here, inner = pl.ds(start, ROWS), pl.ds(pl.multiple_of(start + PAD, 8), ROWS)
            for f in (0, 1):
                p = own_plane[f]
                to_near = g_v[f, here, :] + 0.5 * rx_v[f, 1, j, at, :]
                to_far = rx_v[f, 2, j, at, :] + 0.5 * k_v[p, inner, :]
                step = rx_v[f, 0, j, at, :] - e_v[p, inner, :]
                push = to_far * step
                d_v[f, j, at, :] = -push
                here_half = h_v[p, inner, :] + to_near * step
                far_half = rx_v[f, 3, j, at, :] - push
                h_v[p, inner, :] = here_half
                step = far_half - here_half
                near_v[f, j, at, :] = to_near * step
                fix = -(to_far * step)
                far_v[f, j, at, :] = fix
                sums.append(carry[f] + folded(fix))
            return tuple(sums)

        spill = lax.fori_loop(0, tiles, body, spill)
        for f in (1, 0):
            copy = send(d_v.at[f, j], c_v.at[1 - f, j], s2.at[f, j], r2.at[1 - f, j], neighbour[f])
            copy.start()
            second.append(copy)
        if j < halves - 1:
            ahead(j)

    def fix_copies(act):
        for j in range(halves):
            for f in (0, 1):
                far_place, far_block = lax.rem(side_slab[f], peers), lax.div(side_slab[f], peers)
                slot = lax.div(far_place, 2)
                for c in range(gy_n):
                    at_home = (mine[j] == gx) & (gy == c) & (far_block == gz)
                    act(
                        at_home, far_v.at[f, j, :, lanes(c)], corr.at[slot, 1 - f], sc.at[f, j, c],
                        rc.at[slot, 1 - f], {"gx": mine[j], "gy": jnp.int32(c), "gz": far_block},
                    )

    def begin(at_home, src, dst, send_sem, recv_sem, target):
        @pl.when(at_home)
        def _():
            pltpu.make_async_copy(src, dst, recv_sem).start()

        @pl.when(jnp.logical_not(at_home))
        def _():
            send(src, dst, send_sem, recv_sem, target).start()

    def finish(at_home, src, dst, send_sem, recv_sem, target):
        @pl.when(jnp.logical_not(at_home))
        def _():
            send(src, dst, send_sem, recv_sem, target).wait_send()

    fix_copies(begin)
    ahead(halves - 1)

    def hand_out(block, j, own, act):
        for c in range(gy_n):
            at_home = (block == gx) & (gy == c)
            act(
                at_home, n_v.at[:, pl.ds(row(block), height), lanes(c)], out.at[pl.ds(place * planes, planes)],
                s3.at[2 * j + own, c], r3.at[place], {"gx": block, "gy": jnp.int32(c), "gz": gz},
            )

    for j in range(halves):
        for f in (0, 1):
            first[f, 3, j].wait_send()
            send(d_v.at[f, j], c_v.at[f, j], s2.at[f, j], r2.at[f, j], neighbour[f]).wait_recv()

        @pl.loop(0, tiles)
        def _(t, j=j):
            at = pl.ds(pl.multiple_of(t * ROWS, 8), ROWS)
            inner = pl.ds(pl.multiple_of(theirs[j] * height + t * ROWS + PAD, 8), ROWS)
            for f in (0, 1):
                h_v[own_plane[f], inner, :] = h_v[own_plane[f], inner, :] + c_v[f, j, at, :]

        for p in range(planes):
            second_step(theirs[j], j, 0, p, 0, tiles)
        if j < halves - 1:
            hand_out(theirs[j], j, 0, begin)
    for j in range(halves):
        behind(j)

    spot = lax.broadcasted_iota(jnp.int32, (8, 128), 1)
    scale = 1.0 / (nx * ny)
    part = jnp.zeros((8, 128), jnp.float32)
    base = place * planes
    amounts = [jnp.sum(spill[0], keepdims=True)] + [jnp.sum(s, keepdims=True) for s in sums]
    amounts.append(jnp.sum(spill[1], keepdims=True))
    for i, amount in enumerate(amounts):
        part = jnp.where(spot == base + i, amount * scale, part)
    group_v[0] = part
    share = []
    for i in range(1, peers):
        copy = send(group_v.at[0], group_v.at[i], s4.at[i], r4.at[i], peer(i))
        copy.start()
        share.append(copy)
    hand_out(theirs[-1], halves - 1, 0, begin)
    for j in range(halves):
        hand_out(mine[j], j, 1, begin)
    for copy in share:
        copy.wait_recv()
    for i in range(1, peers):
        part = part + group_v[i]
    block_v[0] = part
    climb = []
    for i in range(1, gz_n):
        copy = send(block_v.at[0], block_v.at[i], s5.at[i], r5.at[i], layer(i))
        copy.start()
        climb.append(copy)
    for copy in climb:
        copy.wait_recv()
    lower = jnp.zeros((8, 128), jnp.float32)
    own_lane = (spot >= 1) & (spot <= count)
    means = jnp.where(own_lane, part, 0.0)
    for i in range(gz_n):
        vector = block_v[i]
        block = lax.rem(gz + gz_n - i, gz_n)
        owner = jnp.where(own_lane, block, jnp.where(
            spot == 0, lax.rem(block + gz_n - 1, gz_n), lax.rem(block + 1, gz_n)))
        vector = jnp.where(spot <= count + 1, vector, 0.0)
        lower = lower + jnp.where(owner < gz, vector, 0.0)
        low = jnp.sum(jnp.where((spot == 0) & (owner == gz), vector, 0.0)[0:1], axis=1, keepdims=True)
        high = jnp.sum(jnp.where((spot == count + 1) & (owner == gz), vector, 0.0)[0:1], axis=1, keepdims=True)
        means = means + jnp.where(spot == count, low, 0.0) + jnp.where(spot == 1, high, 0.0)
    means = pltpu.roll(means, 127, 1)
    running = means
    step = 1
    while step < count:
        running = running + jnp.where(spot >= step, pltpu.roll(running, step, 1), 0.0)
        step *= 2
    mean_ref[...] = means
    offset = jnp.sum(lower[0:1], axis=1, keepdims=True)
    rank = (gz * count + spot + 1).astype(jnp.float32)
    run_ref[...] = (running + offset) / rank

    for s in range(peers):
        dst = out.at[pl.ds(s * planes, planes)]
        send(dst, dst, s3.at[0, 0], r3.at[s], neighbour[0]).wait_recv()
    for slot in range(peers // 2):
        for f in (0, 1):
            send(corr.at[slot, f], corr.at[slot, f], sc.at[0, 0, 0], rc.at[slot, f], neighbour[0]).wait_recv()
    for j in range(halves):
        hand_out(theirs[j], j, 0, finish)
        hand_out(mine[j], j, 1, finish)
    fix_copies(finish)
    for key, copy in first.items():
        if key[1] != 3:
            copy.wait_send()
    for copy in second + share + climb:
        copy.wait_send()


def finish_kernel(planes, base_ref, corr_ref, mean_in, run_in, out_ref, mean_ref, run_ref, fix_v, done):
    other = 1 - lax.rem(lax.axis_index("gx"), 2)
    copies = []
    for slot in range(corr_ref.shape[0]):
        whole = pl.ds((2 * slot + 1 - other) * planes, planes)
        copies.append(pltpu.make_async_copy(base_ref.at[whole], out_ref.at[whole], done.at[slot, 0]))
        copies[-1].start()
    for slot in range(corr_ref.shape[0]):
        start = (2 * slot + other) * planes
        fix_v[slot] = base_ref[pl.ds(start, planes)]
        for f, p in ((0, 0), (1, planes - 1)):
            fix_v[slot, p] = fix_v[slot, p] + corr_ref[slot, f]
        copies.append(pltpu.make_async_copy(fix_v.at[slot], out_ref.at[pl.ds(start, planes)], done.at[slot, 1]))
        copies[-1].start()
    count = mean_ref.shape[0]
    mean_ref[...] = mean_in[0, 0:count]
    run_ref[...] = run_in[0, 0:count]
    for copy in copies:
        copy.wait()


def by_parity(energy, flow):
    gx_n, gy_n, gz_n = (lax.axis_size(a) for a in ("gx", "gy", "gz"))
    planes, nx, ny = energy.shape
    peers, halves = gx_n * gy_n, gx_n // 2
    height, width = nx // gx_n, ny // gy_n
    dma = pltpu.SemaphoreType.DMA
    f32 = jnp.float32
    anywhere = pl.BlockSpec(memory_space=pl.ANY)
    vmem = pl.BlockSpec(memory_space=pltpu.VMEM)
    tall = pltpu.VMEM((planes, nx + 2 * PAD, ny), f32)
    hbm = pl.BlockSpec(memory_space=pltpu.HBM)
    faces = pltpu.VMEM((2, halves, height, ny), f32)
    energy, flow = (pltpu.with_memory_space_constraint(x, pltpu.HBM) for x in (energy, flow))
    base, corr, means, running = pl.pallas_call(
        functools.partial(split_kernel, (gx_n, gy_n, gz_n, planes, nx, ny)),
        out_shape=(
            jax.ShapeDtypeStruct((planes * peers, height, width), f32),
            jax.ShapeDtypeStruct((peers // 2, 2, height, width), f32),
            jax.ShapeDtypeStruct((8, 128), f32),
            jax.ShapeDtypeStruct((8, 128), f32),
        ),
        in_specs=[hbm, hbm],
        out_specs=(anywhere, anywhere, vmem, vmem),
        scratch_shapes=[
            tall, tall, pltpu.VMEM((3, planes, nx, ny), f32), tall,
            pltpu.VMEM((planes, nx, ny), f32), pltpu.VMEM((2, nx, ny), f32),
            pltpu.VMEM((2, 4, halves, height, ny), f32), faces, faces, faces, faces,
            pltpu.VMEM((peers, 8, 128), f32), pltpu.VMEM((gz_n, 8, 128), f32),
            dma((3,)), dma((2, 4, halves)), dma((2, 4, halves)), dma((2, halves)), dma((2, halves)),
            dma((gx_n, gy_n)), dma((peers,)), dma((2, halves, gy_n)), dma((peers // 2, 2)),
            dma((peers,)), dma((peers,)), dma((gz_n,)), dma((gz_n,)),
        ],
        compiler_params=pltpu.CompilerParams(
            collective_id=0, has_side_effects=True, vmem_limit_bytes=12 * (energy.size + flow.size)
        ),
    )(energy, flow)
    count = planes * peers
    return tuple(pl.pallas_call(
        functools.partial(finish_kernel, planes),
        out_shape=(
            jax.ShapeDtypeStruct((count, height, width), f32),
            jax.ShapeDtypeStruct((count,), f32),
            jax.ShapeDtypeStruct((count,), f32),
        ),
        in_specs=[vmem] * 4,
        out_specs=(pl.BlockSpec(memory_space=pltpu.HBM), vmem, vmem),
        scratch_shapes=[pltpu.VMEM((peers // 2, planes, height, width), f32), dma((peers // 2, 2))],
        compiler_params=pltpu.CompilerParams(vmem_limit_bytes=12 * (energy.size + flow.size)),
    )(base, corr, means, running))


def per_device(energy, flow):
    gx_n, gy_n, gz_n = (lax.axis_size(a) for a in ("gx", "gy", "gz"))
    planes, nx, ny = energy.shape
    if planes > 1 and gx_n % 2 == 0 and gz_n > 1:
        return by_parity(energy, flow)
    peers = gx_n * gy_n
    parts = (1 if planes > 2 else 0) + (2 if planes > 1 else 1)
    dma = pltpu.SemaphoreType.DMA
    f32 = jnp.float32
    anywhere = pl.BlockSpec(memory_space=pl.ANY)
    vmem = pl.BlockSpec(memory_space=pltpu.VMEM)
    tall = pltpu.VMEM((planes + 2, nx + 2 * PAD, ny), f32)
    energy_next, means, running = pl.pallas_call(
        functools.partial(kernel, (gx_n, gy_n, gz_n, planes, nx, ny)),
        out_shape=(
            jax.ShapeDtypeStruct((planes * peers, nx // gx_n, ny // gy_n), f32),
            jax.ShapeDtypeStruct((8, 128), f32),
            jax.ShapeDtypeStruct((8, 128), f32),
        ),
        in_specs=[anywhere, anywhere],
        out_specs=(anywhere, vmem, vmem),
        scratch_shapes=[
            tall, tall, pltpu.VMEM((3, planes, nx, ny), f32), tall,
            pltpu.VMEM((planes, nx, ny), f32),
            pltpu.VMEM((peers, 8, 128), f32), pltpu.VMEM((gz_n, 8, 128), f32),
            dma((3,)), dma((gy_n, 4)), dma((gy_n, 4)), dma((gy_n, 2)), dma((gy_n, 2)),
            dma((peers, parts)), dma((peers, parts)), dma((parts,)),
            dma((peers,)), dma((peers,)), dma((gz_n,)), dma((gz_n,)),
        ],
        compiler_params=pltpu.CompilerParams(collective_id=0, has_side_effects=True),
    )(energy, flow)
    count = planes * peers
    return energy_next, means[0, :count], running[0, :count]


def solution(mesh):
    placed = (P(("gz", "gy", "gx"), None, None), P(None, ("gz", "gy", "gx"), None, None))
    return jax.shard_map(
        per_device,
        mesh=mesh,
        in_specs=placed,
        out_specs=(P("gz", "gx", "gy"), P("gz"), P("gz")),
        check_vma=False,
    )
```
